768 devices in a mesh: section: 2 (over core), mp: 8 (over y_lo, x), dp: 48 (over z, y_hi).
Axes of the slice: x: 4, y: 8 (y_hi: 4, y_lo: 2; y = y_hi * 2 + y_lo), z: 12, core: 2. Of those that a mesh axis runs over, the one named last changes fastest.
Arguments:
- value_grad: bfloat16 [2, 24576, 3072], P('section', 'dp', 'mp'), may hold values from -6 to 6
- stream: bfloat16 [2, 24576, 3072], P('section', 'dp'), may hold values from -300 to 300
- weights: bfloat16 [2, 3072, 3072], P('section', 'mp'), may hold values from -0.109375 to 0.109375
- gain: float32 [2, 3072], P('section'), may hold values from 0.25 to 1.75
- top_grad: bfloat16 [24576, 3072], P('dp'), may hold values from -6 to 6
- counts: int32 [48], P('dp'), may hold values from 1 to 2, as said below
Outputs:
- weight_grad: bfloat16 [2, 3072, 3072], P('section', ('mp', 'dp'))
- residual_grad: bfloat16 [2, 24576, 3072], P('section', 'dp', 'mp')
The draws below stay inside these ranges and needn't reach their ends.
Inputs may be any that keep to these rules, and one draw needn't show every extreme that they name: counts[r] counts the live micro-batches of replica r; some replica has all 2.
All inputs are finite; a program needn't handle non-finite values.
Results may differ from the reference program's by a relative error of at most 0.009.
Values may be sent and summed in bfloat16 or wider, within the bound.
No kernel may reach another device: no remote copies, remote signals or barrier semaphores. Data moves between devices by JAX's collectives and lax.ppermute only.
A program may use at most 64 MiB of HBM per device.

```python
import jax
import jax.numpy as jnp
from jax import lax

D = 3072
F = 3072
MICRO = 2
TOK_MB = 256
GROUPS = 8
REPLICAS = 48
TOKENS = 24576


def draw_stream(key, part):
    first, second, third = jax.random.split(key, 3)
    row_scale = jnp.exp(jax.random.uniform(second, (2, TOKENS, 1), jnp.float32) * jnp.log(10.0))
    col_scale = jnp.exp(jax.random.uniform(third, (2, 1, D), jnp.float32) * jnp.log(10.0))
    base = jax.random.normal(first, (2, TOKENS, D), jnp.float32)
    values = jnp.clip(base * row_scale * col_scale * 0.3, -300.0, 300.0)
    return values.astype(jnp.bfloat16)


def draw_counts(key, part):
    first, second = jax.random.split(jax.random.fold_in(key, 7))
    drawn = jax.random.randint(first, (REPLICAS,), 1, MICRO + 1)
    chosen = jax.random.randint(second, (), 0, REPLICAS)
    drawn = drawn.at[chosen].set(MICRO)
    return drawn.astype(jnp.int32)


def strengthened(entries, rng, source, target, shards_of, factor):
    def block_of(position):
        return (jnp.arange(entries.shape[position]) // (entries.shape[position] // shards_of)).reshape((-1,) + (1,) * (entries.ndim - 1 - position))

    near = jax.random.permutation(rng, shards_of)[block_of(target)]
    second = (block_of(target) + shards_of // 2) % shards_of
    return jnp.where((block_of(source) == near) | (block_of(source) == second), factor * entries, entries)


def shard_levels(own_key, extent, shards, least, top_value):
    def one(position, shards_of):
        steps = jax.random.uniform(jax.random.fold_in(jax.random.fold_in(own_key, 6), position), (shards_of,), jnp.float32, least / len(shards), top_value / len(shards))
        return jnp.repeat(jnp.exp(steps), extent[position] // shards_of).reshape((-1,) + (1,) * (len(extent) - position - 1))

    loudness = one(*shards[0])
    for cut in shards[1:]:
        loudness = loudness * one(*cut)
    return loudness


def noise(rng, dims, deviation, reach, shards=(), kind=jnp.bfloat16):
    array = jax.random.normal(rng, dims, jnp.float32) * deviation
    if len(shards) > 0:
        array = shard_levels(rng, dims, shards, -0.22, 0.18) * array
    return jnp.clip(array, min=-reach, max=reach).astype(kind)


def gaussian_with(stream_key, shape, scale, bound, cuts, heavy, kind=jnp.bfloat16):
    entries = scale * jax.random.normal(stream_key, shape, jnp.float32)
    if cuts:
        entries = entries * shard_levels(stream_key, shape, cuts, -0.22, 0.18)
    return jnp.clip(strengthened(entries, jax.random.fold_in(stream_key, 3), *heavy), -bound, bound).astype(kind)


def setup_inputs(seed: int = 0) -> dict:
    seeds = jax.random.split(jax.random.key(seed), 7)
    value_grad = gaussian_with(seeds[0], (2, TOKENS, F), 1.0, 6.0, ((0, 2), (1, 48), (2, 8)), (1, 2, 48, 3.25))
    stream = draw_stream(jax.random.fold_in(seeds[6], 71), 0)
    weights = noise(seeds[2], (2, F, D), D ** -0.5, 0.109375, ((0, 2), (1, 8)))
    gain = jnp.clip(1.0 + 0.15 * jax.random.normal(seeds[3], (2, D), jnp.float32), 0.25, 1.75)
    top_grad = noise(seeds[4], (TOKENS, D), 1.0, 6.0, ((0, 48),))
    counts = draw_counts(jax.random.fold_in(seeds[6], 71), 0)
    return {"value_grad": value_grad, "stream": stream, "weights": weights, "gain": gain, "top_grad": top_grad, "counts": counts}


def normalize(stream_rows):
    values = stream_rows.astype(jnp.float32)
    average = lax.optimization_barrier(jnp.mean(values, axis=-1, keepdims=True))
    centred = values - average
    variance = lax.optimization_barrier(jnp.mean(centred * centred, axis=-1, keepdims=True))
    inv_scale = lax.rsqrt(variance + 1e-06)
    return (centred * inv_scale, inv_scale)

def reference(value_grad, stream, weights, gain, top_grad, counts):
    per_replica = MICRO * TOK_MB
    token_index = jnp.arange(TOKENS, dtype=jnp.int32)
    replica = token_index // per_replica
    micro_index = token_index % per_replica // TOK_MB
    live_mask = (micro_index < counts[replica]).astype(jnp.bfloat16)
    block_rows = F // GROUPS
    weight_grads = []
    branch_terms = []
    for section_index in range(2):
        whitened, inv_scale = normalize(stream[section_index])
        gain_row = gain[section_index].astype(jnp.float32)
        normed = (whitened * gain_row).astype(jnp.bfloat16)
        masked = value_grad[section_index] * live_mask[:, None]
        weight_grads.append(jnp.dot(masked.T, normed, preferred_element_type=jnp.float32).astype(jnp.bfloat16))
        norm_grad = jnp.zeros((TOKENS, D), jnp.float32)
        for block_index in range(GROUPS):
            low = block_index * block_rows
            partial_value = jnp.dot(value_grad[section_index][:, low:low + block_rows], weights[section_index][low:low + block_rows], preferred_element_type=jnp.float32).astype(jnp.bfloat16)
            norm_grad = norm_grad + lax.optimization_barrier(partial_value).astype(jnp.float32)
        scaled_grad = norm_grad * gain_row
        first_mean = lax.optimization_barrier(jnp.mean(scaled_grad, axis=-1, keepdims=True))
        second_mean = lax.optimization_barrier(jnp.mean(scaled_grad * whitened, axis=-1, keepdims=True))
        branch_terms.append(inv_scale * (scaled_grad - first_mean - whitened * second_mean))
    above_grad = (top_grad.astype(jnp.float32) + branch_terms[1]).astype(jnp.bfloat16)
    lower_grad = (above_grad.astype(jnp.float32) + branch_terms[0]).astype(jnp.bfloat16)
    return (jnp.stack(weight_grads), jnp.stack([lower_grad, above_grad]))
```

```python
import jax
import jax.numpy as jnp
from jax import lax
from jax.sharding import Mesh
from jax.sharding import PartitionSpec as P

TOK_MB = 256
DP = ("dz", "dy")
MP = ("my", "mx")
F32 = jnp.float32
BF16 = jnp.bfloat16


def turned(value, axis, by):
    peers = lax.axis_size(axis)
    return lax.ppermute(value, axis, [(i, (i + by) % peers) for i in range(peers)])


def normalize(stream_rows):
    values = stream_rows.astype(F32)
    average = jnp.mean(values, axis=-1, keepdims=True)
    centred = values - average
    variance = jnp.mean(centred * centred, axis=-1, keepdims=True)
    inv_scale = lax.rsqrt(variance + 1e-06)
    return (centred * inv_scale, inv_scale)


def joined(own, got):
    return own.astype(F32) + got.astype(F32)


def sum_over_z(grad):
    peers = lax.axis_size("dz")
    place = lax.axis_index("dz")
    rows = grad.shape[0] // peers
    half = grad.shape[1] // 2
    far = peers // 2

    def block(offset):
        return lax.dynamic_slice_in_dim(grad, ((place + offset) % peers) * rows, rows, 0)

    up = turned(block(far)[:, :half].astype(BF16), "dz", 1)
    down = turned(block(-far)[:, half:].astype(BF16), "dz", -1)
    for k in range(far - 1, 0, -1):
        mine_up = block(k)
        mine_down = block(-k)
        if k == far - 1:
            mine_up = jnp.concatenate([joined(mine_up[:, :half], up), mine_up[:, half:]], axis=1)
            mine_down = jnp.concatenate([mine_down[:, :half], joined(mine_down[:, half:], down)], axis=1)
        else:
            mine_up = joined(mine_up, up)
            mine_down = joined(mine_down, down)
        up = turned(mine_up.astype(BF16), "dz", 1)
        down = turned(mine_down.astype(BF16), "dz", -1)
    return block(0) + up.astype(F32) + down.astype(F32)


def sum_over_y(rows_sum):
    peers = lax.axis_size("dy")
    place = lax.axis_index("dy")
    rows = rows_sum.shape[0] // peers

    def block(offset):
        return lax.dynamic_slice_in_dim(rows_sum, ((place + offset) % peers) * rows, rows, 0)

    got = [turned(block(k).astype(BF16), "dy", k) for k in range(1, peers)]
    total = block(0)
    for g in got:
        total = total + g.astype(F32)
    return total


def sum_at_owner(partial, width):
    x = lax.axis_index("mx")
    y = lax.axis_index("my")

    def part(rx, ry):
        start = (((y + ry) % 2) * 4 + (x + rx) % 4) * width
        return lax.dynamic_slice_in_dim(partial, start, width, 1)

    far_up = turned(part(2, 1), "mx", 1)
    far_down = turned(part(2, 0), "mx", -1)
    near_up = turned(part(1, 0), "mx", 1)
    near_down = turned(part(3, 1), "mx", -1)
    sum_up = turned(joined(part(1, 1), far_up).astype(BF16), "mx", 1)
    sum_down = turned(joined(part(3, 0), far_down).astype(BF16), "mx", -1)
    other = part(0, 1).astype(F32) + near_down.astype(F32) + sum_up.astype(F32)
    across = turned(other.astype(BF16), "my", 1)
    return part(0, 0).astype(F32) + near_up.astype(F32) + sum_down.astype(F32) + across.astype(F32)


def sum_over_mp(value):
    got = [turned(value, "mx", k) for k in range(1, 4)]
    value = value + got[0] + got[1] + got[2]
    return value + turned(value, "my", 1)


def shards(value_grad, stream, weights, gain, top_grad, counts):
    section_index = lax.axis_index("section")
    model_index = lax.axis_index(MP)
    row_total = stream.shape[1]
    width = stream.shape[2]
    share_width = width // lax.axis_size(MP)
    first_col = model_index * share_width
    partial = jnp.dot(value_grad[0], weights[0], preferred_element_type=F32).astype(BF16)
    norm_grad = sum_at_owner(partial, share_width)
    whitened, inv_scale = normalize(stream[0])
    gain_row = gain[0]
    normed = (whitened * gain_row).astype(BF16)
    micro_index = jnp.arange(row_total, dtype=jnp.int32) // TOK_MB
    live_mask = (micro_index < counts[0]).astype(BF16)
    masked = value_grad[0] * live_mask[:, None]
    grad = lax.dot_general(masked, normed, (((0,), (0,)), ((), ())), preferred_element_type=F32)
    weight_grad = sum_over_y(sum_over_z(grad)).astype(BF16)[None]
    scaled_part = partial.astype(F32) * gain_row
    totals = sum_over_mp(jnp.stack([jnp.sum(scaled_part, axis=1), jnp.sum(scaled_part * whitened, axis=1)]))
    white_share = lax.dynamic_slice_in_dim(whitened, first_col, share_width, 1)
    gain_share = lax.dynamic_slice_in_dim(gain_row, first_col, share_width, 0)
    scaled_grad = norm_grad * gain_share
    norm_back = inv_scale * (
        scaled_grad - totals[0][:, None] / width - white_share * (totals[1][:, None] / width)
    )
    top_slice = lax.dynamic_slice_in_dim(top_grad, first_col, share_width, 1).astype(F32)
    above_grad = (top_slice + norm_back).astype(BF16)
    below_grad = lax.ppermute(above_grad, "section", [(1, 0)])
    lower_grad = (below_grad.astype(F32) + norm_back).astype(BF16)
    result = jnp.where(section_index == 0, lower_grad, above_grad)
    return (weight_grad, result[None])


def solution(mesh):
    split = Mesh(
        mesh.devices.reshape(mesh.shape["section"], 2, 4, 12, 4),
        ("section", "my", "mx", "dz", "dy"),
    )
    placed = (
        P("section", DP, MP),
        P("section", DP, None),
        P("section", MP, None),
        P("section", None),
        P(DP, None),
        P(DP),
    )
    return jax.shard_map(
        shards,
        mesh=split,
        in_specs=placed,
        out_specs=(P("section", MP + DP, None), P("section", DP, MP)),
        check_vma=False,
    )
```

```python
import jax
import jax.numpy as jnp
from jax import lax
from jax.sharding import Mesh
from jax.sharding import PartitionSpec as P

TOK_MB = 256
DP = ("dz", "dy")
MP = ("my", "mx")
F32 = jnp.float32
BF16 = jnp.bfloat16


def turned(value, axis, by):
    peers = lax.axis_size(axis)
    return lax.ppermute(value, axis, [(i, (i + by) % peers) for i in range(peers)])


def normalize(stream_rows):
    values = stream_rows.astype(F32)
    average = jnp.mean(values, axis=-1, keepdims=True)
    centred = values - average
    variance = jnp.mean(centred * centred, axis=-1, keepdims=True)
    inv_scale = lax.rsqrt(variance + 1e-06)
    return (centred * inv_scale, inv_scale)


def joined(own, got):
    return own.astype(F32) + got.astype(F32)


def tied(value, *others):
    return lax.optimization_barrier((value, *others))[0]


def sum_over_z(grad, start_between):
    peers = lax.axis_size("dz")
    place = lax.axis_index("dz")
    rows = grad.shape[0] // peers
    far = peers // 2

    def block(offset):
        return lax.dynamic_slice_in_dim(grad, ((place + offset) % peers) * rows, rows, 0)

    with jax.named_scope("up6"):
        up = turned(block(far).astype(BF16), "dz", 1)
    down = None
    for k in range(far - 1, 0, -1):
        if down is not None:
            up, down = lax.optimization_barrier((up, down))
        mine = joined(block(k), up).astype(BF16)
        with jax.named_scope(f"up{k}"):
            up = turned(mine, "dz", 1)
        mine = block(-k).astype(BF16) if down is None else joined(block(-k), down).astype(BF16)
        with jax.named_scope(f"down{k}"):
            down = turned(mine, "dz", -1)
    return block(0) + up.astype(F32) + down.astype(F32)


def sum_over_y(rows_sum):
    peers = lax.axis_size("dy")
    tiles = rows_sum.astype(BF16).reshape(peers, rows_sum.shape[0] // peers, rows_sum.shape[1])
    arrived = lax.all_to_all(tiles, "dy", split_axis=0, concat_axis=0, tiled=True)
    return arrived.astype(F32).sum(axis=0)


def halves(value):
    high = value.astype(BF16)
    return (high, (value - high.astype(F32)).astype(BF16))


def shards(value_grad, stream, weights, gain, top_grad, counts):
    section_index = lax.axis_index("section")
    model_index = lax.axis_index(MP)
    row_total = stream.shape[1]
    width = stream.shape[2]
    share_width = width // lax.axis_size(MP)
    first_col = model_index * share_width
    whitened, inv_scale = normalize(stream[0])
    gain_row = gain[0]
    normed = (whitened * gain_row).astype(BF16)
    micro_index = jnp.arange(row_total, dtype=jnp.int32) // TOK_MB
    live_mask = (micro_index < counts[0]).astype(BF16)
    masked = value_grad[0] * live_mask[:, None]
    grad = lax.dot_general(masked, normed, (((0,), (0,)), ((), ())), preferred_element_type=F32)
    weight_grad = sum_over_y(sum_over_z(grad, None)).astype(BF16)[None]
    partial = jnp.dot(value_grad[0], weights[0], preferred_element_type=F32).astype(BF16)
    scaled_part = partial.astype(F32) * gain_row
    first = jnp.sum(scaled_part, axis=1)
    second = jnp.sum(scaled_part * whitened, axis=1)
    extra = jnp.stack(halves(first) + halves(second))
    extra = jnp.concatenate([extra[:, :384], jnp.pad(extra[:, 384:], ((0, 0), (0, 256)))], axis=0)
    tiles = jnp.moveaxis(partial.reshape(row_total, 8, share_width), 1, 0)
    tiles = jnp.concatenate([tiles, jnp.broadcast_to(extra, (8, 8, share_width))], axis=1)
    with jax.named_scope("parts"):
        arrived = lax.all_to_all(tiles, MP, split_axis=0, concat_axis=0, tiled=True)
    norm_grad = arrived[:, :row_total].astype(F32).sum(axis=0)
    sums = arrived[:, row_total:].astype(F32).sum(axis=0)
    sums = jnp.concatenate([sums[:4], sums[4:, :128]], axis=1)
    totals = (sums[0] + sums[1], sums[2] + sums[3])
    white_share = lax.dynamic_slice_in_dim(whitened, first_col, share_width, 1)
    gain_share = lax.dynamic_slice_in_dim(gain_row, first_col, share_width, 0)
    scaled_grad = norm_grad * gain_share
    norm_back = inv_scale * (
        scaled_grad - totals[0][:, None] / width - white_share * (totals[1][:, None] / width)
    )
    top_slice = lax.dynamic_slice_in_dim(top_grad, first_col, share_width, 1).astype(F32)
    above_grad = (top_slice + norm_back).astype(BF16)
    below_grad = lax.ppermute(above_grad, "section", [(1, 0)])
    lower_grad = (below_grad.astype(F32) + norm_back).astype(BF16)
    result = jnp.where(section_index == 0, lower_grad, above_grad)
    return (weight_grad, result[None])


def solution(mesh):
    split = Mesh(
        mesh.devices.reshape(mesh.shape["section"], 2, 4, 12, 4),
        ("section", "my", "mx", "dz", "dy"),
    )
    placed = (
        P("section", DP, MP),
        P("section", DP, None),
        P("section", MP, None),
        P("section", None),
        P(DP, None),
        P(DP),
    )
    return jax.shard_map(
        shards,
        mesh=split,
        in_specs=placed,
        out_specs=(P("section", MP + DP, None), P("section", DP, MP)),
        check_vma=False,
    )
```

```python
import jax
import jax.numpy as jnp
from jax import lax
from jax.experimental import pallas as pl
from jax.experimental.pallas import tpu as pltpu
from jax.sharding import Mesh
from jax.sharding import PartitionSpec as P


TOK_MB = 256
DP = ("dz", "dy")
MP = ("my", "mx")
F32 = jnp.float32
BF16 = jnp.bfloat16
TOK = 512
BLOCK = 128
CHUNK = 16
WIDTH = 3072
SHARE = 384
RING = 12
ROWS = SHARE // RING
PARTS = 8
EXTRA = 8
COLS = 512


def in_hbm(*arrays):
    return [pltpu.with_memory_space_constraint(a, pltpu.HBM) for a in arrays]


def front_kernel(scal, stream, value_grad, gain, white, scale, average, own, *rest):
    blocks, (normed, masked, grad) = rest[:-3], rest[-3:]
    step = pl.program_id(0)
    base = step * BLOCK
    gains = gain[...]

    def chunk(i, carry):
        rows = pl.ds(pl.multiple_of(i * CHUNK, CHUNK), CHUNK)
        values = stream[rows, :].astype(F32)
        mean = jnp.sum(values, axis=1, keepdims=True) * (1.0 / WIDTH)
        centred = values - mean
        variance = jnp.sum(centred * centred, axis=1, keepdims=True) * (1.0 / WIDTH)
        inv = lax.rsqrt(variance + 1e-06)
        at = pl.ds(pl.multiple_of(base + i * CHUNK, CHUNK), CHUNK)
        normed[at, :] = (centred * inv * gains).astype(BF16)
        scale[rows, :] = inv
        average[rows, :] = mean
        return carry

    lax.fori_loop(0, BLOCK // CHUNK, chunk, 0, unroll=2)
    share = stream[:, pl.ds(pl.multiple_of(scal[2] * SHARE, 128), SHARE)].astype(F32)
    white[...] = (share - average[...]) * scale[...]
    live = jnp.where(base // TOK_MB < scal[3], 1.0, 0.0)
    masked[pl.ds(pl.multiple_of(base, BLOCK), BLOCK), :] = (value_grad[...].astype(F32) * live).astype(BF16)

    @pl.when(step == TOK // BLOCK - 1)
    def _():
        left = masked[...].T
        for n in range(WIDTH // COLS):
            cols = slice(n * COLS, (n + 1) * COLS)
            grad[...] = jnp.dot(left, normed[:, cols], preferred_element_type=F32)
            for r in range(RING):
                at = lax.rem(scal[0] + r * scal[1] + RING, RING) * ROWS
                piece = grad[pl.ds(pl.multiple_of(at, ROWS), ROWS), :]
                if r == 0:
                    own[:, cols] = piece
                else:
                    blocks[r - 1][:, cols] = piece.astype(BF16)


def front(scal, stream, value_grad, gain):
    token = lambda width: pl.BlockSpec((BLOCK, width), lambda i, s: (i, 0))
    whole = lambda shape: pl.BlockSpec(shape, lambda i, s: (0,) * len(shape))
    out = [((TOK, SHARE), F32), ((TOK, 1), F32), ((TOK, 1), F32), ((ROWS, WIDTH), F32)]
    out += [((ROWS, WIDTH), BF16)] * (RING - 1)
    return pl.pallas_call(
        front_kernel,
        grid_spec=pltpu.PrefetchScalarGridSpec(
            num_scalar_prefetch=1,
            grid=(TOK // BLOCK,),
            in_specs=[token(WIDTH), token(SHARE), whole((1, WIDTH))],
            out_specs=[token(SHARE), token(1), token(1)] + [whole((ROWS, WIDTH))] * RING,
            scratch_shapes=[
                pltpu.VMEM((TOK, WIDTH), BF16),
                pltpu.VMEM((TOK, SHARE), BF16),
                pltpu.VMEM((SHARE, COLS), F32),
            ],
        ),
        out_shape=[jax.ShapeDtypeStruct(*o) if i == 3 + RING // 2 else pltpu.HBM(*o) for i, o in enumerate(out)],
        compiler_params=pltpu.CompilerParams(
            dimension_semantics=("arbitrary",), vmem_limit_bytes=40 * 1024 * 1024
        ),
        cost_estimate=pl.CostEstimate(flops=2 * TOK * SHARE * WIDTH * 4, transcendentals=0, bytes_accessed=8_000_000),
    )(scal, *in_hbm(stream, value_grad, gain))


def parts_kernel(value_grad, weights, stream, gain, scale, average, out, held, extra, first, second, sems):
    m = pl.program_id(0)

    @pl.when(m == 0)
    def _():
        first[...] = jnp.zeros_like(first)
        second[...] = jnp.zeros_like(second)

    part = jnp.dot(value_grad[...], weights[...], preferred_element_type=F32).astype(BF16)
    held[m] = part
    copy = pltpu.make_async_copy(held.at[m], out.at[m, pl.ds(0, TOK), :], sems.at[m])
    copy.start()
    scaled = part.astype(F32) * gain[...]
    product = scaled * ((stream[...].astype(F32) - average[...]) * scale[...])
    first[...] += scaled[:, :128] + scaled[:, 128:256] + scaled[:, 256:]
    second[...] += product[:, :128] + product[:, 128:256] + product[:, 256:]

    @pl.when(m == PARTS - 1)
    def _():
        lines = []
        for total in (first, second):
            line = jnp.sum(total[...].T, axis=0, keepdims=True)
            high = line.astype(BF16).astype(F32)
            lines += [high, line - high]
        stacked = jnp.concatenate(lines, axis=0)
        tail = jnp.concatenate([stacked[:, SHARE:], jnp.zeros((4, SHARE - 128), F32)], axis=1)
        extra[...] = jnp.concatenate([stacked[:, :SHARE], tail], axis=0).astype(BF16)
        ends = []
        for j in range(PARTS):
            end = pltpu.make_async_copy(extra, out.at[j, pl.ds(TOK, EXTRA), :], sems.at[PARTS + j])
            end.start()
            ends.append(end)
        for j in range(PARTS):
            pltpu.make_async_copy(held.at[j], out.at[j, pl.ds(0, TOK), :], sems.at[j]).wait()
            ends[j].wait()


def parts(value_grad, weights, stream, gain, scale, average):
    whole = lambda shape: pl.BlockSpec(shape, lambda m: (0,) * len(shape))
    cols = lambda rows: pl.BlockSpec((rows, SHARE), lambda m: (0, m))
    return pl.pallas_call(
        parts_kernel,
        grid=(PARTS,),
        in_specs=[whole((TOK, SHARE)), cols(SHARE), cols(TOK), cols(1), whole((TOK, 1)), whole((TOK, 1))],
        out_specs=pl.BlockSpec(memory_space=pl.ANY),
        out_shape=pltpu.HBM((PARTS, TOK + EXTRA, SHARE), BF16),
        scratch_shapes=[
            pltpu.VMEM((PARTS, TOK, SHARE), BF16),
            pltpu.VMEM((EXTRA, SHARE), BF16),
            pltpu.VMEM((TOK, 128), F32),
            pltpu.VMEM((TOK, 128), F32),
            pltpu.SemaphoreType.DMA((2 * PARTS,)),
        ],
        compiler_params=pltpu.CompilerParams(
            dimension_semantics=("arbitrary",), vmem_limit_bytes=24 * 1024 * 1024
        ),
        cost_estimate=pl.CostEstimate(flops=2 * TOK * SHARE * WIDTH * 3, transcendentals=0, bytes_accessed=9_000_000),
    )(value_grad, weights, stream, gain, scale, average)


def back_kernel(scal, arrived, extra, white, scale, gain, top, back, above, columns):
    step = pl.program_id(0)

    @pl.when(step == 0)
    def _():
        sums = jnp.sum(extra[...].astype(F32), axis=0)
        lines = jnp.concatenate([sums[:4], sums[4:, :128]], axis=1)
        for j, line in enumerate((lines[0:1] + lines[1:2], lines[2:3] + lines[3:4])):
            for b in range(TOK // BLOCK):
                square = jnp.broadcast_to(line[:, b * BLOCK : (b + 1) * BLOCK], (BLOCK, BLOCK))
                columns[j, b * BLOCK : (b + 1) * BLOCK, :] = square.T * (1.0 / WIDTH)

    rows = pl.ds(pl.multiple_of(step * BLOCK, BLOCK), BLOCK)
    mean = columns[0, rows, :][:, :1]
    slope = columns[1, rows, :][:, :1]
    total = arrived[0].astype(F32)
    for j in range(1, PARTS):
        total = total + arrived[j].astype(F32)
    branch = scale[...] * (total * gain[...] - mean - white[...] * slope)
    back[...] = branch
    above[...] = (top[...].astype(F32) + branch).astype(BF16)


def backward(scal, arrived, white, scale, gain, top):
    token = lambda width: pl.BlockSpec((BLOCK, width), lambda i, s: (i, 0))
    return pl.pallas_call(
        back_kernel,
        grid_spec=pltpu.PrefetchScalarGridSpec(
            num_scalar_prefetch=1,
            grid=(TOK // BLOCK,),
            in_specs=[
                pl.BlockSpec((PARTS, BLOCK, SHARE), lambda i, s: (0, i, 0)),
                pl.BlockSpec((PARTS, EXTRA, SHARE), lambda i, s: (0, TOK // EXTRA, 0)),
                token(SHARE),
                token(1),
                pl.BlockSpec((1, SHARE), lambda i, s: (0, s[2])),
                pl.BlockSpec((BLOCK, SHARE), lambda i, s: (i, s[2])),
            ],
            out_specs=[token(SHARE), token(SHARE)],
            scratch_shapes=[pltpu.VMEM((2, TOK, BLOCK), F32)],
        ),
        out_shape=[jax.ShapeDtypeStruct((TOK, SHARE), F32), jax.ShapeDtypeStruct((TOK, SHARE), BF16)],
        compiler_params=pltpu.CompilerParams(
            dimension_semantics=("arbitrary",), vmem_limit_bytes=16 * 1024 * 1024
        ),
        cost_estimate=pl.CostEstimate(flops=500_000_000, transcendentals=0, bytes_accessed=6_000_000),
    )(scal, *in_hbm(arrived, arrived, white, scale, gain, top))


def swapped(value, axis, first):
    peers = lax.axis_size(axis)
    pairs = []
    for i in range(first, peers, 2):
        pairs += [(i, (i + 1) % peers), ((i + 1) % peers, i)]
    return lax.ppermute(value, axis, pairs)


def tied(value, *others):
    return lax.optimization_barrier((value, *others))[0]


def joined(own, got):
    return (own.astype(F32) + got.astype(F32)).astype(BF16)


def sum_over_z(own, blocks):
    def block(link, distance):
        return blocks[(distance if link == 0 else RING - distance) - 1]

    far = RING // 2
    long = swapped(block(0, far), "dz", 0)
    short = None
    link = 0
    for k in range(far - 1, 0, -1):
        link = 1 - link
        if short is None:
            mine_short = tied(block(1 - link, k), long)
        else:
            mine_short = joined(block(1 - link, k), tied(short, long))
        mine = joined(block(link, k), long)
        long = swapped(mine, "dz", link)
        short = swapped(mine_short, "dz", 1 - link)
    return own + long.astype(F32) + short.astype(F32)


def sum_over_y(rows_sum):
    peers = lax.axis_size("dy")
    tiles = rows_sum.astype(BF16).reshape(peers, rows_sum.shape[0] // peers, rows_sum.shape[1])
    arrived = lax.all_to_all(tiles, "dy", split_axis=0, concat_axis=0, tiled=True)
    return arrived.astype(F32).sum(axis=0)


def shards(value_grad, stream, weights, gain, top_grad, counts):
    section_index = lax.axis_index("section")
    model_index = lax.axis_index(MP)
    place = lax.axis_index("dz")
    scal = jnp.stack([place, 1 - 2 * (place % 2), model_index, counts[0]]).astype(jnp.int32)
    white, scale, average, own, *blocks = front(scal, stream[0], value_grad[0], gain)
    weight_grad = sum_over_y(sum_over_z(own, blocks)).astype(BF16)[None]
    tiles = parts(value_grad[0], weights[0], stream[0], gain, scale, average)
    arrived = lax.all_to_all(tiles, MP, split_axis=0, concat_axis=0, tiled=True)
    norm_back, above_grad = backward(scal, arrived, white, scale, gain, top_grad)
    below_grad = lax.ppermute(above_grad, "section", [(1, 0)])
    lower_grad = (below_grad.astype(F32) + norm_back).astype(BF16)
    result = jnp.where(section_index == 0, lower_grad, above_grad)
    return (weight_grad, result[None])


def solution(mesh):
    split = Mesh(
        mesh.devices.reshape(mesh.shape["section"], 2, 4, 12, 4),
        ("section", "my", "mx", "dz", "dy"),
    )
    placed = (
        P("section", DP, MP),
        P("section", DP, None),
        P("section", MP, None),
        P("section", None),
        P(DP, None),
        P(DP),
    )

    return jax.shard_map(
        shards,
        mesh=split,
        in_specs=placed,
        out_specs=(P("section", MP + DP, None), P("section", DP, MP)),
        check_vma=False,
    )
```

```python
import jax
import jax.numpy as jnp
from jax import lax
from jax.experimental import pallas as pl
from jax.experimental.pallas import tpu as pltpu
from jax.sharding import Mesh
from jax.sharding import PartitionSpec as P


TOK_MB = 256
DP = ("dz", "dy")
MP = ("my", "mx")
F32 = jnp.float32
BF16 = jnp.bfloat16
TOK = 512
BLOCK = 128
CHUNK = 16
WIDTH = 3072
SHARE = 384
RING = 12
ROWS = SHARE // RING
PARTS = 8
EXTRA = 8
COLS = 512


def in_hbm(*arrays):
    return [pltpu.with_memory_space_constraint(a, pltpu.HBM) for a in arrays]


def front_kernel(scal, stream, value_grad, gain, white, scale, average, own, *rest):
    blocks, (normed, masked, grad) = rest[:-3], rest[-3:]
    step = pl.program_id(0)
    base = step * BLOCK
    gains = gain[...]

    def chunk(i, carry):
        rows = pl.ds(pl.multiple_of(i * CHUNK, CHUNK), CHUNK)
        values = stream[rows, :].astype(F32)
        mean = jnp.sum(values, axis=1, keepdims=True) * (1.0 / WIDTH)
        centred = values - mean
        variance = jnp.sum(centred * centred, axis=1, keepdims=True) * (1.0 / WIDTH)
        inv = lax.rsqrt(variance + 1e-06)
        at = pl.ds(pl.multiple_of(base + i * CHUNK, CHUNK), CHUNK)
        normed[at, :] = (centred * inv * gains).astype(BF16)
        scale[rows, :] = inv
        average[rows, :] = mean
        return carry

    lax.fori_loop(0, BLOCK // CHUNK, chunk, 0, unroll=2)
    share = stream[:, pl.ds(pl.multiple_of(scal[2] * SHARE, 128), SHARE)].astype(F32)
    white[...] = (share - average[...]) * scale[...]
    live = jnp.where(base // TOK_MB < scal[3], 1.0, 0.0)
    masked[pl.ds(pl.multiple_of(base, BLOCK), BLOCK), :] = (value_grad[...].astype(F32) * live).astype(BF16)

    @pl.when(step == TOK // BLOCK - 1)
    def _():
        left = masked[...].T
        for n in range(WIDTH // COLS):
            cols = slice(n * COLS, (n + 1) * COLS)
            grad[...] = jnp.dot(left, normed[:, cols], preferred_element_type=F32)
            for r in range(RING):
                at = lax.rem(scal[0] + r * scal[1] + RING, RING) * ROWS
                piece = grad[pl.ds(pl.multiple_of(at, ROWS), ROWS), :]
                if r == 0:
                    own[:, cols] = piece
                else:
                    blocks[r - 1][:, cols] = piece.astype(BF16)


def front(scal, stream, value_grad, gain):
    token = lambda width: pl.BlockSpec((BLOCK, width), lambda i, s: (i, 0))
    whole = lambda shape: pl.BlockSpec(shape, lambda i, s: (0,) * len(shape))
    out = [((TOK, SHARE), F32), ((TOK, 1), F32), ((TOK, 1), F32), ((ROWS, WIDTH), F32)]
    out += [((ROWS, WIDTH), BF16)] * (RING - 1)
    return pl.pallas_call(
        front_kernel,
        grid_spec=pltpu.PrefetchScalarGridSpec(
            num_scalar_prefetch=1,
            grid=(TOK // BLOCK,),
            in_specs=[token(WIDTH), token(SHARE), whole((1, WIDTH))],
            out_specs=[token(SHARE), token(1), token(1)] + [whole((ROWS, WIDTH))] * RING,
            scratch_shapes=[
                pltpu.VMEM((TOK, WIDTH), BF16),
                pltpu.VMEM((TOK, SHARE), BF16),
                pltpu.VMEM((SHARE, COLS), F32),
            ],
        ),
        out_shape=[jax.ShapeDtypeStruct(*o) if i == 3 + RING // 2 else pltpu.HBM(*o) for i, o in enumerate(out)],
        compiler_params=pltpu.CompilerParams(
            dimension_semantics=("arbitrary",), vmem_limit_bytes=40 * 1024 * 1024
        ),
        cost_estimate=pl.CostEstimate(flops=2 * TOK * SHARE * WIDTH * 4, transcendentals=0, bytes_accessed=8_000_000),
    )(scal, *in_hbm(stream, value_grad, gain))


def parts_kernel(value_grad, weights, stream, gain, scale, average, out, held, extra, first, second, sems):
    m = pl.program_id(0)

    @pl.when(m == 0)
    def _():
        first[...] = jnp.zeros_like(first)
        second[...] = jnp.zeros_like(second)

    part = jnp.dot(value_grad[...], weights[...], preferred_element_type=F32).astype(BF16)
    held[m] = part
    copy = pltpu.make_async_copy(held.at[m], out.at[m, pl.ds(0, TOK), :], sems.at[m])
    copy.start()
    scaled = part.astype(F32) * gain[...]
    product = scaled * ((stream[...].astype(F32) - average[...]) * scale[...])
    first[...] += scaled[:, :128] + scaled[:, 128:256] + scaled[:, 256:]
    second[...] += product[:, :128] + product[:, 128:256] + product[:, 256:]

    @pl.when(m == PARTS - 1)
    def _():
        lines = []
        for total in (first, second):
            line = jnp.sum(total[...].T, axis=0, keepdims=True)
            high = line.astype(BF16).astype(F32)
            lines += [high, line - high]
        stacked = jnp.concatenate(lines, axis=0)
        tail = jnp.concatenate([stacked[:, SHARE:], jnp.zeros((4, SHARE - 128), F32)], axis=1)
        extra[...] = jnp.concatenate([stacked[:, :SHARE], tail], axis=0).astype(BF16)
        ends = []
        for j in range(PARTS):
            end = pltpu.make_async_copy(extra, out.at[j, pl.ds(TOK, EXTRA), :], sems.at[PARTS + j])
            end.start()
            ends.append(end)
        for j in range(PARTS):
            pltpu.make_async_copy(held.at[j], out.at[j, pl.ds(0, TOK), :], sems.at[j]).wait()
            ends[j].wait()


def parts(value_grad, weights, stream, gain, scale, average):
    whole = lambda shape: pl.BlockSpec(shape, lambda m: (0,) * len(shape))
    cols = lambda rows: pl.BlockSpec((rows, SHARE), lambda m: (0, m))
    return pl.pallas_call(
        parts_kernel,
        grid=(PARTS,),
        in_specs=[whole((TOK, SHARE)), cols(SHARE), cols(TOK), cols(1), whole((TOK, 1)), whole((TOK, 1))],
        out_specs=pl.BlockSpec(memory_space=pl.ANY),
        out_shape=pltpu.HBM((PARTS, TOK + EXTRA, SHARE), BF16),
        scratch_shapes=[
            pltpu.VMEM((PARTS, TOK, SHARE), BF16),
            pltpu.VMEM((EXTRA, SHARE), BF16),
            pltpu.VMEM((TOK, 128), F32),
            pltpu.VMEM((TOK, 128), F32),
            pltpu.SemaphoreType.DMA((2 * PARTS,)),
        ],
        compiler_params=pltpu.CompilerParams(
            dimension_semantics=("arbitrary",), vmem_limit_bytes=24 * 1024 * 1024
        ),
        cost_estimate=pl.CostEstimate(flops=2 * TOK * SHARE * WIDTH * 3, transcendentals=0, bytes_accessed=9_000_000),
    )(value_grad, weights, stream, gain, scale, average)


def back_kernel(scal, arrived, extra, white, scale, gain, top, back, above, columns):
    step = pl.program_id(0)

    @pl.when(step == 0)
    def _():
        sums = jnp.sum(extra[...].astype(F32), axis=0)
        lines = jnp.concatenate([sums[:4], sums[4:, :128]], axis=1)
        for j, line in enumerate((lines[0:1] + lines[1:2], lines[2:3] + lines[3:4])):
            for b in range(TOK // BLOCK):
                square = jnp.broadcast_to(line[:, b * BLOCK : (b + 1) * BLOCK], (BLOCK, BLOCK))
                columns[j, b * BLOCK : (b + 1) * BLOCK, :] = square.T * (1.0 / WIDTH)

    rows = pl.ds(pl.multiple_of(step * BLOCK, BLOCK), BLOCK)
    mean = columns[0, rows, :][:, :1]
    slope = columns[1, rows, :][:, :1]
    total = arrived[0].astype(F32)
    for j in range(1, PARTS):
        total = total + arrived[j].astype(F32)
    branch = scale[...] * (total * gain[...] - mean - white[...] * slope)
    back[...] = branch
    above[...] = (top[...].astype(F32) + branch).astype(BF16)


def backward(scal, arrived, white, scale, gain, top):
    token = lambda width: pl.BlockSpec((BLOCK, width), lambda i, s: (i, 0))
    return pl.pallas_call(
        back_kernel,
        grid_spec=pltpu.PrefetchScalarGridSpec(
            num_scalar_prefetch=1,
            grid=(TOK // BLOCK,),
            in_specs=[
                pl.BlockSpec((PARTS, BLOCK, SHARE), lambda i, s: (0, i, 0)),
                pl.BlockSpec((PARTS, EXTRA, SHARE), lambda i, s: (0, TOK // EXTRA, 0)),
                token(SHARE),
                token(1),
                pl.BlockSpec((1, SHARE), lambda i, s: (0, s[2])),
                pl.BlockSpec((BLOCK, SHARE), lambda i, s: (i, s[2])),
            ],
            out_specs=[token(SHARE), token(SHARE)],
            scratch_shapes=[pltpu.VMEM((2, TOK, BLOCK), F32)],
        ),
        out_shape=[jax.ShapeDtypeStruct((TOK, SHARE), F32), jax.ShapeDtypeStruct((TOK, SHARE), BF16)],
        compiler_params=pltpu.CompilerParams(
            dimension_semantics=("arbitrary",), vmem_limit_bytes=16 * 1024 * 1024
        ),
        cost_estimate=pl.CostEstimate(flops=500_000_000, transcendentals=0, bytes_accessed=6_000_000),
    )(scal, *in_hbm(arrived, arrived, white, scale, gain, top))


def swapped(value, link):
    peers = lax.axis_size("dz")
    pairs = []
    for section in range(2):
        for i in range((link + section) % 2, peers, 2):
            here, there = section * peers + i, section * peers + (i + 1) % peers
            pairs += [(here, there), (there, here)]
    return lax.ppermute(value, ("section", "dz"), pairs)


def tied(value, *others):
    return lax.optimization_barrier((value, *others))[0]


def joined(own, got):
    return (own.astype(F32) + got.astype(F32)).astype(BF16)


def sum_over_z(own, blocks):
    def block(link, distance):
        return blocks[(distance if link == 0 else RING - distance) - 1]

    far = RING // 2
    long = swapped(block(0, far), 0)
    short = None
    link = 0
    for k in range(far - 1, 0, -1):
        link = 1 - link
        if short is None:
            mine_short = tied(block(1 - link, k), long)
        else:
            mine_short = joined(block(1 - link, k), tied(short, long))
        mine = joined(block(link, k), long)
        long = swapped(mine, link)
        short = swapped(mine_short, 1 - link)
    return own + long.astype(F32) + short.astype(F32)


def sum_over_y(rows_sum):
    peers = lax.axis_size("dy")
    tiles = rows_sum.astype(BF16).reshape(peers, rows_sum.shape[0] // peers, rows_sum.shape[1])
    arrived = lax.all_to_all(tiles, "dy", split_axis=0, concat_axis=0, tiled=True)
    return arrived.astype(F32).sum(axis=0)


def shards(value_grad, stream, weights, gain, top_grad, counts):
    section_index = lax.axis_index("section")
    model_index = lax.axis_index(MP)
    place = lax.axis_index("dz")
    scal = jnp.stack([place, 1 - 2 * ((place + section_index) % 2), model_index, counts[0]]).astype(jnp.int32)
    white, scale, average, own, *blocks = front(scal, stream[0], value_grad[0], gain)
    weight_grad = sum_over_y(sum_over_z(own, blocks)).astype(BF16)[None]
    tiles = parts(value_grad[0], weights[0], stream[0], gain, scale, average)
    arrived = lax.all_to_all(tiles, MP, split_axis=0, concat_axis=0, tiled=True)
    norm_back, above_grad = backward(scal, arrived, white, scale, gain, top_grad)
    below_grad = lax.ppermute(above_grad, "section", [(1, 0)])
    lower_grad = (below_grad.astype(F32) + norm_back).astype(BF16)
    result = jnp.where(section_index == 0, lower_grad, above_grad)
    return (weight_grad, result[None])


def solution(mesh):
    split = Mesh(
        mesh.devices.reshape(mesh.shape["section"], 2, 4, 12, 4),
        ("section", "my", "mx", "dz", "dy"),
    )
    placed = (
        P("section", DP, MP),
        P("section", DP, None),
        P("section", MP, None),
        P("section", None),
        P(DP, None),
        P(DP),
    )

    return jax.shard_map(
        shards,
        mesh=split,
        in_specs=placed,
        out_specs=(P("section", MP + DP, None), P("section", DP, MP)),
        check_vma=False,
    )
```

```python
import jax
import jax.numpy as jnp
from jax import lax
from jax.experimental import pallas as pl
from jax.experimental.pallas import tpu as pltpu
from jax.sharding import Mesh
from jax.sharding import PartitionSpec as P


TOK_MB = 256
DP = ("dz", "dy")
MP = ("my", "mx")
F32 = jnp.float32
BF16 = jnp.bfloat16
TOK = 512
BLOCK = 128
CHUNK = 16
UNROLL = 8
WIDTH = 3072
SHARE = 384
RING = 12
ROWS = SHARE // RING
PARTS = 8
EXTRA = 8
COLS = 512


def in_hbm(*arrays):
    return [pltpu.with_memory_space_constraint(a, pltpu.HBM) for a in arrays]


def front_kernel(scal, stream, value_grad_from, gain_from, held, stats, own, *rest):
    blocks, (normed, grad, value_grad, gain, sems) = rest[:-5], rest[-5:]
    per = TOK // BLOCK
    gain_here = pltpu.make_async_copy(gain_from, gain, sems.at[per])
    gain_here.start()
    arrivals = []
    for b in range(TOK // BLOCK):
        rows = pl.ds(b * BLOCK, BLOCK)
        arrivals.append(pltpu.make_async_copy(stream.at[rows, :], held.at[rows, :], sems.at[b]))
        arrivals[-1].start()
    value_grad_here = pltpu.make_async_copy(value_grad_from, value_grad, sems.at[per + 1])
    value_grad_here.start()
    gain_here.wait()
    lanes = [slice(t * 128, (t + 1) * 128) for t in range(WIDTH // 128)]

    def chunk(i, carry):
        rows = pl.ds(pl.multiple_of(i * CHUNK, CHUNK), CHUNK)
        total = [jnp.zeros((CHUNK, 128), F32)] * 2
        for t, lane in enumerate(lanes):
            total[t % 2] += held[rows, lane].astype(F32)
        mean = jnp.sum(total[0] + total[1], axis=1, keepdims=True) * (1.0 / WIDTH)
        total = [jnp.zeros((CHUNK, 128), F32)] * 2
        for t, lane in enumerate(lanes):
            centred = held[rows, lane].astype(F32) - mean
            total[t % 2] += centred * centred
        variance = jnp.sum(total[0] + total[1], axis=1, keepdims=True) * (1.0 / WIDTH)
        inv = lax.rsqrt(variance + 1e-06)
        for lane in lanes:
            normed[rows, lane] = ((held[rows, lane].astype(F32) - mean) * inv * gain[:, lane]).astype(BF16)
        stats[0, rows, :] = jnp.broadcast_to(inv, (CHUNK, 128))
        stats[1, rows, :] = jnp.broadcast_to(mean, (CHUNK, 128))
        return carry

    per = BLOCK // CHUNK
    for b in range(TOK // BLOCK):
        arrivals[b].wait()
        lax.fori_loop(b * per, (b + 1) * per, chunk, 0, unroll=UNROLL)
    value_grad_here.wait()
    token = lax.broadcasted_iota(jnp.int32, (TOK, SHARE), 0)
    live = token < scal[3] * TOK_MB
    left = jnp.where(live, value_grad[...].astype(F32), 0.0).astype(BF16).T
    for n in range(WIDTH // COLS):
        cols = slice(n * COLS, (n + 1) * COLS)
        grad[...] = jnp.dot(left, normed[:, cols], preferred_element_type=F32)
        for r in range(RING):
            at = lax.rem(scal[0] + r * scal[1] + RING, RING) * ROWS
            piece = grad[pl.ds(pl.multiple_of(at, ROWS), ROWS), :]
            if r == 0:
                own[:, cols] = piece
            else:
                blocks[r - 1][:, cols] = piece.astype(BF16)


def front(scal, stream, value_grad, gain):
    vmem = pl.BlockSpec(memory_space=pltpu.VMEM)
    out = [((TOK, WIDTH), BF16), ((2, TOK, 128), F32), ((ROWS, WIDTH), F32)]
    out += [((ROWS, WIDTH), BF16)] * (RING - 1)
    return pl.pallas_call(
        front_kernel,
        in_specs=[
            pl.BlockSpec(memory_space=pltpu.SMEM),
            *[pl.BlockSpec(memory_space=pl.ANY)] * 3,
        ],
        out_specs=[vmem] * len(out),
        scratch_shapes=[
            pltpu.VMEM((TOK, WIDTH), BF16),
            pltpu.VMEM((SHARE, COLS), F32),
            pltpu.VMEM((TOK, SHARE), BF16),
            pltpu.VMEM((1, WIDTH), F32),
            pltpu.SemaphoreType.DMA((TOK // BLOCK + 2,)),
        ],
        out_shape=[jax.ShapeDtypeStruct(*o) for o in out],
        compiler_params=pltpu.CompilerParams(vmem_limit_bytes=24 * 1024 * 1024),
        cost_estimate=pl.CostEstimate(flops=2 * TOK * SHARE * WIDTH * 4, transcendentals=0, bytes_accessed=8_000_000),
    )(scal, *in_hbm(stream, value_grad, gain))


def parts_kernel(value_grad, weights, held, gain, stats, out, packed, extra, sums, sems):
    copies = []
    for m in range(PARTS):
        cols = slice(m * SHARE, (m + 1) * SHARE)
        part = jnp.dot(value_grad[...], weights[:, cols], preferred_element_type=F32).astype(BF16)
        packed[m] = part
        copies.append(pltpu.make_async_copy(packed.at[m], out.at[m, pl.ds(0, TOK), :], sems.at[m]))
        copies[-1].start()
        scaled = part.astype(F32) * gain[:, cols]
        tiles = [scaled[:, t * 128 : (t + 1) * 128] for t in range(SHARE // 128)]
        first = tiles[0] + tiles[1] + tiles[2]
        second = None
        for t, tile in enumerate(tiles):
            low = m * SHARE + t * 128
            term = tile * (held[:, low : low + 128].astype(F32) - stats[1])
            second = term if second is None else second + term
        if m == 0:
            sums[0] = first
            sums[1] = second
        else:
            sums[0] += first
            sums[1] += second
    lines = []
    for total in (sums[0], sums[1] * stats[0]):
        line = jnp.sum(total.T, axis=0, keepdims=True)
        high = line.astype(BF16).astype(F32)
        lines += [high, line - high]
    stacked = jnp.concatenate(lines, axis=0)
    tail = jnp.concatenate([stacked[:, SHARE:], jnp.zeros((4, SHARE - 128), F32)], axis=1)
    extra[...] = jnp.concatenate([stacked[:, :SHARE], tail], axis=0).astype(BF16)
    for m in range(PARTS):
        copies.append(pltpu.make_async_copy(extra, out.at[m, pl.ds(TOK, EXTRA), :], sems.at[PARTS + m]))
        copies[-1].start()
    for copy in copies:
        copy.wait()


def parts(value_grad, weights, held, gain, stats):
    vmem = pl.BlockSpec(memory_space=pltpu.VMEM)
    return pl.pallas_call(
        parts_kernel,
        in_specs=[vmem] * 5,
        out_specs=pl.BlockSpec(memory_space=pl.ANY),
        out_shape=pltpu.HBM((PARTS, TOK + EXTRA, SHARE), BF16),
        scratch_shapes=[
            pltpu.VMEM((PARTS, TOK, SHARE), BF16),
            pltpu.VMEM((EXTRA, SHARE), BF16),
            pltpu.VMEM((2, TOK, 128), F32),
            pltpu.SemaphoreType.DMA((2 * PARTS,)),
        ],
        compiler_params=pltpu.CompilerParams(vmem_limit_bytes=16 * 1024 * 1024),
        cost_estimate=pl.CostEstimate(flops=2 * TOK * SHARE * WIDTH * 3, transcendentals=0, bytes_accessed=9_000_000),
    )(value_grad, weights, held, gain, stats)


def back_kernel(scal, arrived, extra, stream, stats, gain, top, back, above, columns):
    step = pl.program_id(0)

    @pl.when(step == 0)
    def _():
        sums = jnp.sum(extra[...].astype(F32), axis=0)
        lines = jnp.concatenate([sums[:4], sums[4:, :128]], axis=1)
        for j, line in enumerate((lines[0:1] + lines[1:2], lines[2:3] + lines[3:4])):
            for b in range(TOK // BLOCK):
                square = jnp.broadcast_to(line[:, b * BLOCK : (b + 1) * BLOCK], (BLOCK, BLOCK))
                columns[j, b * BLOCK : (b + 1) * BLOCK, :] = square.T * (1.0 / WIDTH)

    rows = pl.ds(pl.multiple_of(step * BLOCK, BLOCK), BLOCK)
    mean = columns[0, rows, :][:, :1]
    slope = columns[1, rows, :][:, :1]
    total = arrived[0].astype(F32)
    for j in range(1, PARTS):
        total = total + arrived[j].astype(F32)
    scale = stats[0][:, 0:1]
    white = (stream[...].astype(F32) - stats[1][:, 0:1]) * scale
    branch = scale * (total * gain[...] - mean - white * slope)
    back[...] = branch
    above[...] = (top[...].astype(F32) + branch).astype(BF16)


def backward(scal, arrived, stream, stats, gain, top):
    token = lambda width: pl.BlockSpec((BLOCK, width), lambda i, s: (i, 0))
    return pl.pallas_call(
        back_kernel,
        grid_spec=pltpu.PrefetchScalarGridSpec(
            num_scalar_prefetch=1,
            grid=(TOK // BLOCK,),
            in_specs=[
                pl.BlockSpec((PARTS, BLOCK, SHARE), lambda i, s: (0, i, 0)),
                pl.BlockSpec((PARTS, EXTRA, SHARE), lambda i, s: (0, TOK // EXTRA, 0)),
                pl.BlockSpec((BLOCK, SHARE), lambda i, s: (i, s[2])),
                pl.BlockSpec((2, BLOCK, 128), lambda i, s: (0, i, 0)),
                pl.BlockSpec((1, SHARE), lambda i, s: (0, s[2])),
                pl.BlockSpec((BLOCK, SHARE), lambda i, s: (i, s[2])),
            ],
            out_specs=[token(SHARE), token(SHARE)],
            scratch_shapes=[pltpu.VMEM((2, TOK, BLOCK), F32)],
        ),
        out_shape=[jax.ShapeDtypeStruct((TOK, SHARE), F32), jax.ShapeDtypeStruct((TOK, SHARE), BF16)],
        compiler_params=pltpu.CompilerParams(
            dimension_semantics=("arbitrary",), vmem_limit_bytes=16 * 1024 * 1024
        ),
        cost_estimate=pl.CostEstimate(flops=500_000_000, transcendentals=0, bytes_accessed=6_000_000),
    )(scal, *in_hbm(arrived, arrived, stream, stats, gain, top))


def swapped(value, link):
    peers = lax.axis_size("dz")
    pairs = []
    for i in range(link, peers, 2):
        pairs += [(i, (i + 1) % peers), ((i + 1) % peers, i)]
    return lax.ppermute(value, "dz", pairs)


def tied(value, *others):
    return lax.optimization_barrier((value, *others))[0]


def joined_kernel(own, got, out):
    out[...] = (own[...].astype(F32) + got[...].astype(F32)).astype(BF16)


def joined(own, got):
    vmem = pl.BlockSpec(memory_space=pltpu.VMEM)
    return pl.pallas_call(
        joined_kernel,
        in_specs=[vmem, vmem],
        out_specs=vmem,
        out_shape=jax.ShapeDtypeStruct(own.shape, BF16),
        compiler_params=pltpu.CompilerParams(vmem_limit_bytes=4 * 1024 * 1024),
    )(own, got)


def sum_over_z(own, blocks):
    def block(link, distance):
        return blocks[(distance if link == 0 else RING - distance) - 1]

    far = RING // 2
    long = swapped(block(0, far), 0)
    short = None
    link = 0
    for k in range(far - 1, 0, -1):
        link = 1 - link
        if short is None:
            mine_short = tied(block(1 - link, k), long)
        else:
            mine_short = joined(block(1 - link, k), tied(short, long))
        mine = joined(block(link, k), long)
        long = swapped(mine, link)
        short = swapped(mine_short, 1 - link)
    return own + long.astype(F32) + short.astype(F32)


def sum_over_y(rows_sum):
    peers = lax.axis_size("dy")
    tiles = rows_sum.astype(BF16).reshape(peers, rows_sum.shape[0] // peers, rows_sum.shape[1])
    arrived = lax.all_to_all(tiles, "dy", split_axis=0, concat_axis=0, tiled=True)
    return arrived.astype(F32).sum(axis=0)


def shards(value_grad, stream, weights, gain, top_grad, counts):
    section_index = lax.axis_index("section")
    model_index = lax.axis_index(MP)
    place = lax.axis_index("dz")
    scal = jnp.stack([place, 1 - 2 * (place % 2), model_index, counts[0]]).astype(jnp.int32)
    held, stats, own, *blocks = front(scal, stream[0], value_grad[0], gain)
    weight_grad = sum_over_y(sum_over_z(own, blocks)).astype(BF16)[None]
    tiles = parts(value_grad[0], weights[0], held, gain, stats)
    arrived = lax.all_to_all(tiles, MP, split_axis=0, concat_axis=0, tiled=True)
    norm_back, above_grad = backward(scal, arrived, stream[0], stats, gain, top_grad)
    below_grad = lax.ppermute(above_grad, "section", [(1, 0)])
    lower_grad = (below_grad.astype(F32) + norm_back).astype(BF16)
    result = jnp.where(section_index == 0, lower_grad, above_grad)
    return (weight_grad, result[None])


def solution(mesh):
    split = Mesh(
        mesh.devices.reshape(mesh.shape["section"], 2, 4, 12, 4),
        ("section", "my", "mx", "dz", "dy"),
    )
    placed = (
        P("section", DP, MP),
        P("section", DP, None),
        P("section", MP, None),
        P("section", None),
        P(DP, None),
        P(DP),
    )

    return jax.shard_map(
        shards,
        mesh=split,
        in_specs=placed,
        out_specs=(P("section", MP + DP, None), P("section", DP, MP)),
        check_vma=False,
    )
```

```python
import functools

import jax
import jax.numpy as jnp
from jax import lax
from jax.experimental import pallas as pl
from jax.experimental.pallas import tpu as pltpu
from jax.sharding import Mesh
from jax.sharding import PartitionSpec as P


TOK_MB = 256
DP = ("dz", "dy")
MP = ("my", "mx")
F32 = jnp.float32
BF16 = jnp.bfloat16
TOK = 512
BLOCK = 128
CHUNK = 16
UNROLL = 8
WIDTH = 3072
SHARE = 384
RING = 12
ROWS = SHARE // RING
PARTS = 8
EXTRA = 8
COLS = 512
HALF = WIDTH // 2
KEEP = (7, 4, 9, 2, 11)
GIVE = (5, 8, 3, 10, 1)


def in_hbm(*arrays):
    return [pltpu.with_memory_space_constraint(a, pltpu.HBM) for a in arrays]


def front_kernel(scal, stream, value_grad_from, gain_from, held, stats, own, *rest):
    keep_half, give_half, keep, give, normed, grad, value_grad, gain, sems = rest
    per = TOK // BLOCK
    gain_here = pltpu.make_async_copy(gain_from, gain, sems.at[per])
    gain_here.start()
    arrivals = []
    for b in range(TOK // BLOCK):
        rows = pl.ds(b * BLOCK, BLOCK)
        arrivals.append(pltpu.make_async_copy(stream.at[rows, :], held.at[rows, :], sems.at[b]))
        arrivals[-1].start()
    value_grad_here = pltpu.make_async_copy(value_grad_from, value_grad, sems.at[per + 1])
    value_grad_here.start()
    gain_here.wait()
    lanes = [slice(t * 128, (t + 1) * 128) for t in range(WIDTH // 128)]

    def chunk(i, carry):
        rows = pl.ds(pl.multiple_of(i * CHUNK, CHUNK), CHUNK)
        total = [jnp.zeros((CHUNK, 128), F32)] * 2
        for t, lane in enumerate(lanes):
            total[t % 2] += held[rows, lane].astype(F32)
        mean = jnp.sum(total[0] + total[1], axis=1, keepdims=True) * (1.0 / WIDTH)
        total = [jnp.zeros((CHUNK, 128), F32)] * 2
        for t, lane in enumerate(lanes):
            centred = held[rows, lane].astype(F32) - mean
            total[t % 2] += centred * centred
        variance = jnp.sum(total[0] + total[1], axis=1, keepdims=True) * (1.0 / WIDTH)
        inv = lax.rsqrt(variance + 1e-06)
        for lane in lanes:
            normed[rows, lane] = ((held[rows, lane].astype(F32) - mean) * inv * gain[:, lane]).astype(BF16)
        stats[0, rows, :] = jnp.broadcast_to(inv, (CHUNK, 128))
        stats[1, rows, :] = jnp.broadcast_to(mean, (CHUNK, 128))
        return carry

    per = BLOCK // CHUNK
    for b in range(TOK // BLOCK):
        arrivals[b].wait()
        lax.fori_loop(b * per, (b + 1) * per, chunk, 0, unroll=UNROLL)
    value_grad_here.wait()
    token = lax.broadcasted_iota(jnp.int32, (TOK, SHARE), 0)
    live = token < scal[3] * TOK_MB
    left = jnp.where(live, value_grad[...].astype(F32), 0.0).astype(BF16).T
    for n in range(WIDTH // COLS):
        cols = slice(n * COLS, (n + 1) * COLS)
        grad[...] = jnp.dot(left, normed[:, cols], preferred_element_type=F32)

        def piece(r):
            at = lax.rem(scal[0] + r * scal[1] + RING, RING) * ROWS
            return grad[pl.ds(pl.multiple_of(at, ROWS), ROWS), :]

        own[:, cols] = piece(0)
        for j, (mine, other) in enumerate(zip(KEEP, GIVE)):
            keep[j, :, cols] = piece(mine).astype(BF16)
            give[j, :, cols] = piece(other).astype(BF16)
        within = slice(n * COLS % HALF, n * COLS % HALF + COLS)
        far = piece(RING // 2).astype(BF16)
        kept = scal[4] == n * COLS // HALF

        @pl.when(kept)
        def _():
            keep_half[:, within] = far

        @pl.when(jnp.logical_not(kept))
        def _():
            give_half[:, within] = far


def front(scal, stream, value_grad, gain):
    vmem = pl.BlockSpec(memory_space=pltpu.VMEM)
    out = [((TOK, WIDTH), BF16), ((2, TOK, 128), F32), ((ROWS, WIDTH), F32)]
    out += [((ROWS, HALF), BF16)] * 2 + [((len(KEEP), ROWS, WIDTH), BF16)] * 2
    return pl.pallas_call(
        front_kernel,
        in_specs=[
            pl.BlockSpec(memory_space=pltpu.SMEM),
            *[pl.BlockSpec(memory_space=pl.ANY)] * 3,
        ],
        out_specs=[vmem] * len(out),
        scratch_shapes=[
            pltpu.VMEM((TOK, WIDTH), BF16),
            pltpu.VMEM((SHARE, COLS), F32),
            pltpu.VMEM((TOK, SHARE), BF16),
            pltpu.VMEM((1, WIDTH), F32),
            pltpu.SemaphoreType.DMA((TOK // BLOCK + 2,)),
        ],
        out_shape=[jax.ShapeDtypeStruct(*o) for o in out],
        compiler_params=pltpu.CompilerParams(vmem_limit_bytes=24 * 1024 * 1024),
        cost_estimate=pl.CostEstimate(flops=2 * TOK * SHARE * WIDTH * 4, transcendentals=0, bytes_accessed=8_000_000),
    )(scal, *in_hbm(stream, value_grad, gain))


def parts_kernel(value_grad, weights, held, gain, stats, out, packed, extra, sums, sems):
    copies = []
    for m in range(PARTS):
        cols = slice(m * SHARE, (m + 1) * SHARE)
        part = jnp.dot(value_grad[...], weights[:, cols], preferred_element_type=F32).astype(BF16)
        packed[m] = part
        copies.append(pltpu.make_async_copy(packed.at[m], out.at[m, pl.ds(0, TOK), :], sems.at[m]))
        copies[-1].start()
        scaled = part.astype(F32) * gain[:, cols]
        tiles = [scaled[:, t * 128 : (t + 1) * 128] for t in range(SHARE // 128)]
        first = tiles[0] + tiles[1] + tiles[2]
        second = None
        for t, tile in enumerate(tiles):
            low = m * SHARE + t * 128
            term = tile * (held[:, low : low + 128].astype(F32) - stats[1])
            second = term if second is None else second + term
        if m == 0:
            sums[0] = first
            sums[1] = second
        else:
            sums[0] += first
            sums[1] += second
    lines = []
    for total in (sums[0], sums[1] * stats[0]):
        line = jnp.sum(total.T, axis=0, keepdims=True)
        high = line.astype(BF16).astype(F32)
        lines += [high, line - high]
    stacked = jnp.concatenate(lines, axis=0)
    tail = jnp.concatenate([stacked[:, SHARE:], jnp.zeros((4, SHARE - 128), F32)], axis=1)
    extra[...] = jnp.concatenate([stacked[:, :SHARE], tail], axis=0).astype(BF16)
    for m in range(PARTS):
        copies.append(pltpu.make_async_copy(extra, out.at[m, pl.ds(TOK, EXTRA), :], sems.at[PARTS + m]))
        copies[-1].start()
    for copy in copies:
        copy.wait()


def parts(value_grad, weights, held, gain, stats):
    vmem = pl.BlockSpec(memory_space=pltpu.VMEM)
    return pl.pallas_call(
        parts_kernel,
        in_specs=[vmem] * 5,
        out_specs=pl.BlockSpec(memory_space=pl.ANY),
        out_shape=pltpu.HBM((PARTS, TOK + EXTRA, SHARE), BF16),
        scratch_shapes=[
            pltpu.VMEM((PARTS, TOK, SHARE), BF16),
            pltpu.VMEM((EXTRA, SHARE), BF16),
            pltpu.VMEM((2, TOK, 128), F32),
            pltpu.SemaphoreType.DMA((2 * PARTS,)),
        ],
        compiler_params=pltpu.CompilerParams(vmem_limit_bytes=16 * 1024 * 1024),
        cost_estimate=pl.CostEstimate(flops=2 * TOK * SHARE * WIDTH * 3, transcendentals=0, bytes_accessed=9_000_000),
    )(value_grad, weights, held, gain, stats)


def back_kernel(scal, arrived, extra, stream, stats, gain, top, back, above, columns):
    step = pl.program_id(0)

    @pl.when(step == 0)
    def _():
        sums = jnp.sum(extra[...].astype(F32), axis=0)
        lines = jnp.concatenate([sums[:4], sums[4:, :128]], axis=1)
        for j, line in enumerate((lines[0:1] + lines[1:2], lines[2:3] + lines[3:4])):
            for b in range(TOK // BLOCK):
                square = jnp.broadcast_to(line[:, b * BLOCK : (b + 1) * BLOCK], (BLOCK, BLOCK))
                columns[j, b * BLOCK : (b + 1) * BLOCK, :] = square.T * (1.0 / WIDTH)

    rows = pl.ds(pl.multiple_of(step * BLOCK, BLOCK), BLOCK)
    mean = columns[0, rows, :][:, :1]
    slope = columns[1, rows, :][:, :1]
    total = arrived[0].astype(F32)
    for j in range(1, PARTS):
        total = total + arrived[j].astype(F32)
    scale = stats[0][:, 0:1]
    white = (stream[...].astype(F32) - stats[1][:, 0:1]) * scale
    branch = scale * (total * gain[...] - mean - white * slope)
    back[...] = branch
    above[...] = (top[...].astype(F32) + branch).astype(BF16)


def backward(scal, arrived, stream, stats, gain, top):
    token = lambda width: pl.BlockSpec((BLOCK, width), lambda i, s: (i, 0))
    return pl.pallas_call(
        back_kernel,
        grid_spec=pltpu.PrefetchScalarGridSpec(
            num_scalar_prefetch=1,
            grid=(TOK // BLOCK,),
            in_specs=[
                pl.BlockSpec((PARTS, BLOCK, SHARE), lambda i, s: (0, i, 0)),
                pl.BlockSpec((PARTS, EXTRA, SHARE), lambda i, s: (0, TOK // EXTRA, 0)),
                pl.BlockSpec((BLOCK, SHARE), lambda i, s: (i, s[2])),
                pl.BlockSpec((2, BLOCK, 128), lambda i, s: (0, i, 0)),
                pl.BlockSpec((1, SHARE), lambda i, s: (0, s[2])),
                pl.BlockSpec((BLOCK, SHARE), lambda i, s: (i, s[2])),
            ],
            out_specs=[token(SHARE), token(SHARE)],
            scratch_shapes=[pltpu.VMEM((2, TOK, BLOCK), F32)],
        ),
        out_shape=[jax.ShapeDtypeStruct((TOK, SHARE), F32), jax.ShapeDtypeStruct((TOK, SHARE), BF16)],
        compiler_params=pltpu.CompilerParams(
            dimension_semantics=("arbitrary",), vmem_limit_bytes=16 * 1024 * 1024
        ),
        cost_estimate=pl.CostEstimate(flops=500_000_000, transcendentals=0, bytes_accessed=6_000_000),
    )(scal, *in_hbm(arrived, arrived, stream, stats, gain, top))


def swapped(value, link):
    peers = lax.axis_size("dz")
    pairs = []
    for section in range(2):
        for i in range((link + section) % 2, peers, 2):
            here, there = section * peers + i, section * peers + (i + 1) % peers
            pairs += [(here, there), (there, here)]
    return lax.ppermute(value, ("section", "dz"), pairs)


def traded(value):
    return lax.ppermute(value, "section", [(0, 1), (1, 0)])


def half_kernel(scal, keep, taken, got, out):
    out[0] = keep[0]
    out[1] = taken[0]
    cols = pl.ds(pl.multiple_of(scal[4] * HALF, 128), HALF)
    out[0, :, cols] = (keep[0, :, cols].astype(F32) + got[0].astype(F32)).astype(BF16)
    out[1, :, cols] = (taken[0, :, cols].astype(F32) + got[1].astype(F32)).astype(BF16)


def whole_kernel(j, scal, keep, taken, got, out):
    out[0] = (keep[j].astype(F32) + got[0].astype(F32)).astype(BF16)
    out[1] = (taken[j].astype(F32) + got[1].astype(F32)).astype(BF16)


def joined(j, scal, keep, taken, got):
    vmem = pl.BlockSpec(memory_space=pltpu.VMEM)
    return pl.pallas_call(
        functools.partial(whole_kernel, j) if j else half_kernel,
        in_specs=[pl.BlockSpec(memory_space=pltpu.SMEM), vmem, vmem, vmem],
        out_specs=vmem,
        out_shape=jax.ShapeDtypeStruct((2, ROWS, WIDTH), BF16),
        compiler_params=pltpu.CompilerParams(vmem_limit_bytes=4 * 1024 * 1024),
    )(scal, keep, taken, got)


def sum_over_z(scal, own, keep_half, give_half, keep, give):
    taken_half = traded(give_half)
    got = swapped(jnp.stack([keep_half, taken_half]), 0)
    taken = traded(give)
    for j in range(len(KEEP)):
        message = joined(j, scal, keep, taken, got)
        got = swapped(message, (j + 1) % 2)
    other = traded(got[1])
    return own + got[0].astype(F32) + other.astype(F32)


def sum_over_y(rows_sum):
    peers = lax.axis_size("dy")
    tiles = rows_sum.astype(BF16).reshape(peers, rows_sum.shape[0] // peers, rows_sum.shape[1])
    arrived = lax.all_to_all(tiles, "dy", split_axis=0, concat_axis=0, tiled=True)
    return arrived.astype(F32).sum(axis=0)


def shards(value_grad, stream, weights, gain, top_grad, counts):
    section_index = lax.axis_index("section")
    model_index = lax.axis_index(MP)
    place = lax.axis_index("dz")
    ahead = 1 - 2 * ((place + section_index) % 2)
    scal = jnp.stack([place, ahead, model_index, counts[0], section_index]).astype(jnp.int32)
    held, stats, *blocks = front(scal, stream[0], value_grad[0], gain)
    weight_grad = sum_over_y(sum_over_z(scal, *blocks)).astype(BF16)[None]
    tiles = parts(value_grad[0], weights[0], held, gain, stats)
    arrived = lax.all_to_all(tiles, MP, split_axis=0, concat_axis=0, tiled=True)
    norm_back, above_grad = backward(scal, arrived, stream[0], stats, gain, top_grad)
    below_grad = lax.ppermute(above_grad, "section", [(1, 0)])
    lower_grad = (below_grad.astype(F32) + norm_back).astype(BF16)
    result = jnp.where(section_index == 0, lower_grad, above_grad)
    return (weight_grad, result[None])


def solution(mesh):
    split = Mesh(
        mesh.devices.reshape(mesh.shape["section"], 2, 4, 12, 4),
        ("section", "my", "mx", "dz", "dy"),
    )
    placed = (
        P("section", DP, MP),
        P("section", DP, None),
        P("section", MP, None),
        P("section", None),
        P(DP, None),
        P(DP),
    )

    return jax.shard_map(
        shards,
        mesh=split,
        in_specs=placed,
        out_specs=(P("section", MP + DP, None), P("section", DP, MP)),
        check_vma=False,
    )
```

```python
import jax
import jax.numpy as jnp
from jax import lax
from jax.experimental import pallas as pl
from jax.experimental.pallas import tpu as pltpu
from jax.sharding import Mesh
from jax.sharding import PartitionSpec as P


TOK_MB = 256
DP = ("dz", "dy")
MP = ("my", "mx")
F32 = jnp.float32
BF16 = jnp.bfloat16
TOK = 512
BLOCK = 128
CHUNK = 16
UNROLL = 8
WIDTH = 3072
SHARE = 384
RING = 12
ROWS = SHARE // RING
PARTS = 8
EXTRA = 8
COLS = 512


def in_hbm(*arrays):
    return [pltpu.with_memory_space_constraint(a, pltpu.HBM) for a in arrays]


def front_kernel(scal, stream, value_grad_from, gain_from, held, stats, own, *rest):
    blocks, (normed, grad, value_grad, gain, sems) = rest[:-5], rest[-5:]
    per = TOK // BLOCK
    gain_here = pltpu.make_async_copy(gain_from, gain, sems.at[per])
    gain_here.start()
    arrivals = []
    for b in range(TOK // BLOCK):
        rows = pl.ds(b * BLOCK, BLOCK)
        arrivals.append(pltpu.make_async_copy(stream.at[rows, :], held.at[rows, :], sems.at[b]))
        arrivals[-1].start()
    value_grad_here = pltpu.make_async_copy(value_grad_from, value_grad, sems.at[per + 1])
    value_grad_here.start()
    gain_here.wait()
    lanes = [slice(t * 128, (t + 1) * 128) for t in range(WIDTH // 128)]

    def chunk(i, carry):
        rows = pl.ds(pl.multiple_of(i * CHUNK, CHUNK), CHUNK)
        total = [jnp.zeros((CHUNK, 128), F32)] * 2
        for t, lane in enumerate(lanes):
            total[t % 2] += held[rows, lane].astype(F32)
        mean = jnp.sum(total[0] + total[1], axis=1, keepdims=True) * (1.0 / WIDTH)
        total = [jnp.zeros((CHUNK, 128), F32)] * 2
        for t, lane in enumerate(lanes):
            centred = held[rows, lane].astype(F32) - mean
            total[t % 2] += centred * centred
        variance = jnp.sum(total[0] + total[1], axis=1, keepdims=True) * (1.0 / WIDTH)
        inv = lax.rsqrt(variance + 1e-06)
        for lane in lanes:
            normed[rows, lane] = ((held[rows, lane].astype(F32) - mean) * inv * gain[:, lane]).astype(BF16)
        stats[0, rows, :] = jnp.broadcast_to(inv, (CHUNK, 128))
        stats[1, rows, :] = jnp.broadcast_to(mean, (CHUNK, 128))
        return carry

    per = BLOCK // CHUNK
    for b in range(TOK // BLOCK):
        arrivals[b].wait()
        lax.fori_loop(b * per, (b + 1) * per, chunk, 0, unroll=UNROLL)
    value_grad_here.wait()
    token = lax.broadcasted_iota(jnp.int32, (TOK, SHARE), 0)
    live = token < scal[3] * TOK_MB
    left = jnp.where(live, value_grad[...].astype(F32), 0.0).astype(BF16).T
    for n in range(WIDTH // COLS):
        cols = slice(n * COLS, (n + 1) * COLS)
        grad[...] = jnp.dot(left, normed[:, cols], preferred_element_type=F32)
        for r in range(RING):
            at = lax.rem(scal[0] + r * scal[1] + RING, RING) * ROWS
            piece = grad[pl.ds(pl.multiple_of(at, ROWS), ROWS), :]
            if r == 0:
                own[:, cols] = piece
            else:
                blocks[r - 1][:, cols] = piece.astype(BF16)


def front(scal, stream, value_grad, gain):
    vmem = pl.BlockSpec(memory_space=pltpu.VMEM)
    out = [((TOK, WIDTH), BF16), ((2, TOK, 128), F32), ((ROWS, WIDTH), F32)]
    out += [((ROWS, WIDTH), BF16)] * (RING - 1)
    return pl.pallas_call(
        front_kernel,
        in_specs=[
            pl.BlockSpec(memory_space=pltpu.SMEM),
            *[pl.BlockSpec(memory_space=pl.ANY)] * 3,
        ],
        out_specs=[vmem] * len(out),
        scratch_shapes=[
            pltpu.VMEM((TOK, WIDTH), BF16),
            pltpu.VMEM((SHARE, COLS), F32),
            pltpu.VMEM((TOK, SHARE), BF16),
            pltpu.VMEM((1, WIDTH), F32),
            pltpu.SemaphoreType.DMA((TOK // BLOCK + 2,)),
        ],
        out_shape=[jax.ShapeDtypeStruct(*o) for o in out],
        compiler_params=pltpu.CompilerParams(vmem_limit_bytes=24 * 1024 * 1024),
        cost_estimate=pl.CostEstimate(flops=2 * TOK * SHARE * WIDTH * 4, transcendentals=0, bytes_accessed=8_000_000),
    )(scal, *in_hbm(stream, value_grad, gain))


def parts_kernel(value_grad, weights, held, gain, stats, out, packed, extra, sums, sems):
    copies = []
    for m in range(PARTS):
        cols = slice(m * SHARE, (m + 1) * SHARE)
        part = jnp.dot(value_grad[...], weights[:, cols], preferred_element_type=F32).astype(BF16)
        packed[m] = part
        copies.append(pltpu.make_async_copy(packed.at[m], out.at[m, pl.ds(0, TOK), :], sems.at[m]))
        copies[-1].start()
        scaled = part.astype(F32) * gain[:, cols]
        tiles = [scaled[:, t * 128 : (t + 1) * 128] for t in range(SHARE // 128)]
        first = tiles[0] + tiles[1] + tiles[2]
        second = None
        for t, tile in enumerate(tiles):
            low = m * SHARE + t * 128
            term = tile * (held[:, low : low + 128].astype(F32) - stats[1])
            second = term if second is None else second + term
        if m == 0:
            sums[0] = first
            sums[1] = second
        else:
            sums[0] += first
            sums[1] += second
    lines = []
    for total in (sums[0], sums[1] * stats[0]):
        line = jnp.sum(total.T, axis=0, keepdims=True)
        high = line.astype(BF16).astype(F32)
        lines += [high, line - high]
    stacked = jnp.concatenate(lines, axis=0)
    tail = jnp.concatenate([stacked[:, SHARE:], jnp.zeros((4, SHARE - 128), F32)], axis=1)
    extra[...] = jnp.concatenate([stacked[:, :SHARE], tail], axis=0).astype(BF16)
    for m in range(PARTS):
        copies.append(pltpu.make_async_copy(extra, out.at[m, pl.ds(TOK, EXTRA), :], sems.at[PARTS + m]))
        copies[-1].start()
    for copy in copies:
        copy.wait()


def parts(value_grad, weights, held, gain, stats):
    vmem = pl.BlockSpec(memory_space=pltpu.VMEM)
    return pl.pallas_call(
        parts_kernel,
        in_specs=[vmem] * 5,
        out_specs=pl.BlockSpec(memory_space=pl.ANY),
        out_shape=pltpu.HBM((PARTS, TOK + EXTRA, SHARE), BF16),
        scratch_shapes=[
            pltpu.VMEM((PARTS, TOK, SHARE), BF16),
            pltpu.VMEM((EXTRA, SHARE), BF16),
            pltpu.VMEM((2, TOK, 128), F32),
            pltpu.SemaphoreType.DMA((2 * PARTS,)),
        ],
        compiler_params=pltpu.CompilerParams(vmem_limit_bytes=16 * 1024 * 1024),
        cost_estimate=pl.CostEstimate(flops=2 * TOK * SHARE * WIDTH * 3, transcendentals=0, bytes_accessed=9_000_000),
    )(value_grad, weights, held, gain, stats)


def back_kernel(scal, arrived, extra, stream, stats, gain, top, back, above, columns):
    step = pl.program_id(0)

    @pl.when(step == 0)
    def _():
        sums = jnp.sum(extra[...].astype(F32), axis=0)
        lines = jnp.concatenate([sums[:4], sums[4:, :128]], axis=1)
        for j, line in enumerate((lines[0:1] + lines[1:2], lines[2:3] + lines[3:4])):
            for b in range(TOK // BLOCK):
                square = jnp.broadcast_to(line[:, b * BLOCK : (b + 1) * BLOCK], (BLOCK, BLOCK))
                columns[j, b * BLOCK : (b + 1) * BLOCK, :] = square.T * (1.0 / WIDTH)

    rows = pl.ds(pl.multiple_of(step * BLOCK, BLOCK), BLOCK)
    mean = columns[0, rows, :][:, :1]
    slope = columns[1, rows, :][:, :1]
    total = arrived[0].astype(F32)
    for j in range(1, PARTS):
        total = total + arrived[j].astype(F32)
    scale = stats[0][:, 0:1]
    white = (stream[...].astype(F32) - stats[1][:, 0:1]) * scale
    branch = scale * (total * gain[...] - mean - white * slope)
    back[...] = branch
    above[...] = (top[...].astype(F32) + branch).astype(BF16)


def backward(scal, arrived, stream, stats, gain, top):
    token = lambda width: pl.BlockSpec((BLOCK, width), lambda i, s: (i, 0))
    return pl.pallas_call(
        back_kernel,
        grid_spec=pltpu.PrefetchScalarGridSpec(
            num_scalar_prefetch=1,
            grid=(TOK // BLOCK,),
            in_specs=[
                pl.BlockSpec((PARTS, BLOCK, SHARE), lambda i, s: (0, i, 0)),
                pl.BlockSpec((PARTS, EXTRA, SHARE), lambda i, s: (0, TOK // EXTRA, 0)),
                pl.BlockSpec((BLOCK, SHARE), lambda i, s: (i, s[2])),
                pl.BlockSpec((2, BLOCK, 128), lambda i, s: (0, i, 0)),
                pl.BlockSpec((1, SHARE), lambda i, s: (0, s[2])),
                pl.BlockSpec((BLOCK, SHARE), lambda i, s: (i, s[2])),
            ],
            out_specs=[token(SHARE), token(SHARE)],
            scratch_shapes=[pltpu.VMEM((2, TOK, BLOCK), F32)],
        ),
        out_shape=[jax.ShapeDtypeStruct((TOK, SHARE), F32), jax.ShapeDtypeStruct((TOK, SHARE), BF16)],
        compiler_params=pltpu.CompilerParams(
            dimension_semantics=("arbitrary",), vmem_limit_bytes=16 * 1024 * 1024
        ),
        cost_estimate=pl.CostEstimate(flops=500_000_000, transcendentals=0, bytes_accessed=6_000_000),
    )(scal, *in_hbm(arrived, arrived, stream, stats, gain, top))


def swapped(value, link):
    peers = lax.axis_size("dz")
    pairs = []
    for i in range(link, peers, 2):
        pairs += [(i, (i + 1) % peers), ((i + 1) % peers, i)]
    return lax.ppermute(value, "dz", pairs)


def tied(value, *others):
    return lax.optimization_barrier((value, *others))[0]


def joined_kernel(own, got, out):
    out[...] = (own[...].astype(F32) + got[...].astype(F32)).astype(BF16)


def joined(own, got):
    vmem = pl.BlockSpec(memory_space=pltpu.VMEM)
    return pl.pallas_call(
        joined_kernel,
        in_specs=[vmem, vmem],
        out_specs=vmem,
        out_shape=jax.ShapeDtypeStruct(own.shape, BF16),
        compiler_params=pltpu.CompilerParams(vmem_limit_bytes=4 * 1024 * 1024),
    )(own, got)


def sum_over_z(own, blocks, after):
    def block(link, distance):
        return blocks[(distance if link == 0 else RING - distance) - 1]

    far = RING // 2
    long = swapped(block(0, far), 0)
    short = None
    link = 0
    for k in range(far - 1, 0, -1):
        link = 1 - link
        if short is None:
            mine_short = tied(block(1 - link, k), after)
        else:
            mine_short = joined(block(1 - link, k), short)
            long = tied(long, short)
        short = swapped(mine_short, 1 - link)
        mine = joined(block(link, k), long)
        long = swapped(mine, link)
    return own + long.astype(F32) + short.astype(F32)


def sum_over_y(rows_sum):
    peers = lax.axis_size("dy")
    tiles = rows_sum.astype(BF16).reshape(peers, rows_sum.shape[0] // peers, rows_sum.shape[1])
    arrived = lax.all_to_all(tiles, "dy", split_axis=0, concat_axis=0, tiled=True)
    return arrived.astype(F32).sum(axis=0)


def shards(value_grad, stream, weights, gain, top_grad, counts):
    section_index = lax.axis_index("section")
    model_index = lax.axis_index(MP)
    place = lax.axis_index("dz")
    scal = jnp.stack([place, 1 - 2 * (place % 2), model_index, counts[0]]).astype(jnp.int32)
    held, stats, own, *blocks = front(scal, stream[0], value_grad[0], gain)
    tiles = parts(value_grad[0], weights[0], held, gain, stats)
    weight_grad = sum_over_y(sum_over_z(own, blocks, tiles)).astype(BF16)[None]
    arrived = lax.all_to_all(tiles, MP, split_axis=0, concat_axis=0, tiled=True)
    norm_back, above_grad = backward(scal, arrived, stream[0], stats, gain, top_grad)
    below_grad = lax.ppermute(above_grad, "section", [(1, 0)])
    lower_grad = (below_grad.astype(F32) + norm_back).astype(BF16)
    result = jnp.where(section_index == 0, lower_grad, above_grad)
    return (weight_grad, result[None])


def solution(mesh):
    split = Mesh(
        mesh.devices.reshape(mesh.shape["section"], 2, 4, 12, 4),
        ("section", "my", "mx", "dz", "dy"),
    )
    placed = (
        P("section", DP, MP),
        P("section", DP, None),
        P("section", MP, None),
        P("section", None),
        P(DP, None),
        P(DP),
    )

    return jax.shard_map(
        shards,
        mesh=split,
        in_specs=placed,
        out_specs=(P("section", MP + DP, None), P("section", DP, MP)),
        check_vma=False,
    )
```

```python
import jax
import jax.numpy as jnp
from jax import lax
from jax.experimental import pallas as pl
from jax.experimental.pallas import tpu as pltpu
from jax.sharding import Mesh
from jax.sharding import PartitionSpec as P


TOK_MB = 256
DP = ("dz", "dy")
MP = ("my", "mx")
F32 = jnp.float32
BF16 = jnp.bfloat16
TOK = 512
BLOCK = 128
CHUNK = 16
UNROLL = 8
WIDTH = 3072
SHARE = 384
RING = 12
ROWS = SHARE // RING
PARTS = 8
EXTRA = 8
COLS = 512


def in_hbm(*arrays):
    return [pltpu.with_memory_space_constraint(a, pltpu.HBM) for a in arrays]


def front_kernel(scal, stream, value_grad_from, gain_from, held, stats, own, *rest):
    blocks, (normed, grad, value_grad, gain, sems) = rest[:-5], rest[-5:]
    per = TOK // BLOCK
    gain_here = pltpu.make_async_copy(gain_from, gain, sems.at[per])
    gain_here.start()
    arrivals = []
    for b in range(TOK // BLOCK):
        rows = pl.ds(b * BLOCK, BLOCK)
        arrivals.append(pltpu.make_async_copy(stream.at[rows, :], held.at[rows, :], sems.at[b]))
        arrivals[-1].start()
    value_grad_here = pltpu.make_async_copy(value_grad_from, value_grad, sems.at[per + 1])
    value_grad_here.start()
    gain_here.wait()
    lanes = [slice(t * 128, (t + 1) * 128) for t in range(WIDTH // 128)]

    def chunk(i, carry):
        rows = pl.ds(pl.multiple_of(i * CHUNK, CHUNK), CHUNK)
        total = [jnp.zeros((CHUNK, 128), F32)] * 2
        for t, lane in enumerate(lanes):
            total[t % 2] += held[rows, lane].astype(F32)
        mean = jnp.sum(total[0] + total[1], axis=1, keepdims=True) * (1.0 / WIDTH)
        total = [jnp.zeros((CHUNK, 128), F32)] * 2
        for t, lane in enumerate(lanes):
            centred = held[rows, lane].astype(F32) - mean
            total[t % 2] += centred * centred
        variance = jnp.sum(total[0] + total[1], axis=1, keepdims=True) * (1.0 / WIDTH)
        inv = lax.rsqrt(variance + 1e-06)
        for lane in lanes:
            normed[rows, lane] = ((held[rows, lane].astype(F32) - mean) * inv * gain[:, lane]).astype(BF16)
        stats[0, rows, :] = jnp.broadcast_to(inv, (CHUNK, 128))
        stats[1, rows, :] = jnp.broadcast_to(mean, (CHUNK, 128))
        return carry

    per = BLOCK // CHUNK
    for b in range(TOK // BLOCK):
        arrivals[b].wait()
        lax.fori_loop(b * per, (b + 1) * per, chunk, 0, unroll=UNROLL)
    value_grad_here.wait()
    token = lax.broadcasted_iota(jnp.int32, (TOK, SHARE), 0)
    live = token < scal[3] * TOK_MB
    left = jnp.where(live, value_grad[...].astype(F32), 0.0).astype(BF16).T
    for n in range(WIDTH // COLS):
        cols = slice(n * COLS, (n + 1) * COLS)
        grad[...] = jnp.dot(left, normed[:, cols], preferred_element_type=F32)
        for r in range(RING):
            at = lax.rem(scal[0] + r * scal[1] + RING, RING) * ROWS
            piece = grad[pl.ds(pl.multiple_of(at, ROWS), ROWS), :]
            if r == 0:
                own[:, cols] = piece
            else:
                blocks[r - 1][:, cols] = piece.astype(BF16)


def front(scal, stream, value_grad, gain):
    vmem = pl.BlockSpec(memory_space=pltpu.VMEM)
    out = [((TOK, WIDTH), BF16), ((2, TOK, 128), F32), ((ROWS, WIDTH), F32)]
    out += [((ROWS, WIDTH), BF16)] * (RING - 1)
    return pl.pallas_call(
        front_kernel,
        in_specs=[
            pl.BlockSpec(memory_space=pltpu.SMEM),
            *[pl.BlockSpec(memory_space=pl.ANY)] * 3,
        ],
        out_specs=[vmem] * len(out),
        scratch_shapes=[
            pltpu.VMEM((TOK, WIDTH), BF16),
            pltpu.VMEM((SHARE, COLS), F32),
            pltpu.VMEM((TOK, SHARE), BF16),
            pltpu.VMEM((1, WIDTH), F32),
            pltpu.SemaphoreType.DMA((TOK // BLOCK + 2,)),
        ],
        out_shape=[jax.ShapeDtypeStruct(*o) for o in out],
        compiler_params=pltpu.CompilerParams(vmem_limit_bytes=24 * 1024 * 1024),
        cost_estimate=pl.CostEstimate(flops=2 * TOK * SHARE * WIDTH * 4, transcendentals=0, bytes_accessed=8_000_000),
    )(scal, *in_hbm(stream, value_grad, gain))


def parts_kernel(value_grad, weights, held, gain, stats, out, packed, extra, sums, sems):
    copies = []
    for m in range(PARTS):
        cols = slice(m * SHARE, (m + 1) * SHARE)
        part = jnp.dot(value_grad[...], weights[:, cols], preferred_element_type=F32).astype(BF16)
        packed[m] = part
        copies.append(pltpu.make_async_copy(packed.at[m], out.at[m, pl.ds(0, TOK), :], sems.at[m]))
        copies[-1].start()
        scaled = part.astype(F32) * gain[:, cols]
        tiles = [scaled[:, t * 128 : (t + 1) * 128] for t in range(SHARE // 128)]
        first = tiles[0] + tiles[1] + tiles[2]
        second = None
        for t, tile in enumerate(tiles):
            low = m * SHARE + t * 128
            term = tile * (held[:, low : low + 128].astype(F32) - stats[1])
            second = term if second is None else second + term
        if m == 0:
            sums[0] = first
            sums[1] = second
        else:
            sums[0] += first
            sums[1] += second
    lines = []
    for total in (sums[0], sums[1] * stats[0]):
        line = jnp.sum(total.T, axis=0, keepdims=True)
        high = line.astype(BF16).astype(F32)
        lines += [high, line - high]
    stacked = jnp.concatenate(lines, axis=0)
    tail = jnp.concatenate([stacked[:, SHARE:], jnp.zeros((4, SHARE - 128), F32)], axis=1)
    extra[...] = jnp.concatenate([stacked[:, :SHARE], tail], axis=0).astype(BF16)
    for m in range(PARTS):
        copies.append(pltpu.make_async_copy(extra, out.at[m, pl.ds(TOK, EXTRA), :], sems.at[PARTS + m]))
        copies[-1].start()
    for copy in copies:
        copy.wait()


def parts(value_grad, weights, held, gain, stats):
    vmem = pl.BlockSpec(memory_space=pltpu.VMEM)
    return pl.pallas_call(
        parts_kernel,
        in_specs=[vmem] * 5,
        out_specs=pl.BlockSpec(memory_space=pl.ANY),
        out_shape=pltpu.HBM((PARTS, TOK + EXTRA, SHARE), BF16),
        scratch_shapes=[
            pltpu.VMEM((PARTS, TOK, SHARE), BF16),
            pltpu.VMEM((EXTRA, SHARE), BF16),
            pltpu.VMEM((2, TOK, 128), F32),
            pltpu.SemaphoreType.DMA((2 * PARTS,)),
        ],
        compiler_params=pltpu.CompilerParams(vmem_limit_bytes=16 * 1024 * 1024),
        cost_estimate=pl.CostEstimate(flops=2 * TOK * SHARE * WIDTH * 3, transcendentals=0, bytes_accessed=9_000_000),
    )(value_grad, weights, held, gain, stats)


def back_kernel(scal, sent, stats, gain, top, stream, back, above, arrived, top_here, stream_here, columns, sems):
    share = pl.ds(pl.multiple_of(scal[2] * SHARE, 128), SHARE)
    fetches = [
        pltpu.make_async_copy(stream.at[:, share], stream_here, sems.at[0]),
        pltpu.make_async_copy(top.at[:, share], top_here, sems.at[1]),
    ]
    rows_of = [pl.ds(TOK, EXTRA)] + [pl.ds(b * BLOCK, BLOCK) for b in range(TOK // BLOCK)]
    for i, rows in enumerate(rows_of):
        fetches.append(pltpu.make_async_copy(sent.at[:, rows, :], arrived.at[:, rows, :], sems.at[2 + i]))
    for i in (2, 0, 1, 3, 4, 5, 6):
        fetches[i].start()
    fetches[2].wait()
    sums = jnp.sum(arrived[:, TOK:, :].astype(F32), axis=0)
    lines = jnp.concatenate([sums[:4], sums[4:, :128]], axis=1)
    for j, line in enumerate((lines[0:1] + lines[1:2], lines[2:3] + lines[3:4])):
        for b in range(TOK // BLOCK):
            square = jnp.broadcast_to(line[:, b * BLOCK : (b + 1) * BLOCK], (BLOCK, BLOCK))
            columns[j, b * BLOCK : (b + 1) * BLOCK, :] = square.T * (1.0 / WIDTH)
    gains = gain[:, share]
    fetches[0].wait()
    fetches[1].wait()

    def chunk(i, carry):
        rows = pl.ds(pl.multiple_of(i * CHUNK, CHUNK), CHUNK)
        total = arrived[0, rows, :].astype(F32)
        for j in range(1, PARTS):
            total = total + arrived[j, rows, :].astype(F32)
        spread = lambda a: jnp.concatenate([a] * (SHARE // 128), axis=1)
        scale = spread(stats[0, rows, :])
        white = (stream_here[rows, :].astype(F32) - spread(stats[1, rows, :])) * scale
        branch = scale * (total * gains - spread(columns[0, rows, :]) - white * spread(columns[1, rows, :]))
        back[rows, :] = branch
        above[rows, :] = (top_here[rows, :].astype(F32) + branch).astype(BF16)
        return carry

    per = BLOCK // CHUNK
    for b in range(TOK // BLOCK):
        fetches[3 + b].wait()
        lax.fori_loop(b * per, (b + 1) * per, chunk, 0, unroll=4)


def backward(scal, arrived, stats, gain, top, stream):
    vmem = pl.BlockSpec(memory_space=pltpu.VMEM)
    hbm = pl.BlockSpec(memory_space=pl.ANY)
    return pl.pallas_call(
        back_kernel,
        in_specs=[pl.BlockSpec(memory_space=pltpu.SMEM), hbm, vmem, vmem, hbm, hbm],
        out_specs=[vmem, vmem],
        scratch_shapes=[
            pltpu.VMEM((PARTS, TOK + EXTRA, SHARE), BF16),
            pltpu.VMEM((TOK, SHARE), BF16),
            pltpu.VMEM((TOK, SHARE), BF16),
            pltpu.VMEM((2, TOK, BLOCK), F32),
            pltpu.SemaphoreType.DMA((2 + 1 + TOK // BLOCK,)),
        ],
        out_shape=[jax.ShapeDtypeStruct((TOK, SHARE), F32), jax.ShapeDtypeStruct((TOK, SHARE), BF16)],
        compiler_params=pltpu.CompilerParams(vmem_limit_bytes=12 * 1024 * 1024),
        cost_estimate=pl.CostEstimate(flops=500_000_000, transcendentals=0, bytes_accessed=6_000_000),
    )(scal, *in_hbm(arrived), stats, gain, *in_hbm(top, stream))


def swapped(value, link):
    peers = lax.axis_size("dz")
    pairs = []
    for i in range(link, peers, 2):
        pairs += [(i, (i + 1) % peers), ((i + 1) % peers, i)]
    return lax.ppermute(value, "dz", pairs)


def tied(value, *others):
    return lax.optimization_barrier((value, *others))[0]


def joined_kernel(own, got, out):
    out[...] = (own[...].astype(F32) + got[...].astype(F32)).astype(BF16)


def joined(own, got):
    vmem = pl.BlockSpec(memory_space=pltpu.VMEM)
    return pl.pallas_call(
        joined_kernel,
        in_specs=[vmem, vmem],
        out_specs=vmem,
        out_shape=jax.ShapeDtypeStruct(own.shape, BF16),
        compiler_params=pltpu.CompilerParams(vmem_limit_bytes=4 * 1024 * 1024),
    )(own, got)


def sum_over_z(own, blocks, after):
    def block(link, distance):
        return blocks[(distance if link == 0 else RING - distance) - 1]

    far = RING // 2
    long = swapped(block(0, far), 0)
    short = None
    link = 0
    for k in range(far - 1, 0, -1):
        link = 1 - link
        if short is None:
            mine_short = tied(block(1 - link, k), after)
        else:
            mine_short = joined(block(1 - link, k), short)
            long = tied(long, short)
        short = swapped(mine_short, 1 - link)
        mine = joined(block(link, k), long)
        long = swapped(mine, link)
    return own + long.astype(F32) + short.astype(F32)


def sum_over_y(rows_sum):
    peers = lax.axis_size("dy")
    tiles = rows_sum.astype(BF16).reshape(peers, rows_sum.shape[0] // peers, rows_sum.shape[1])
    arrived = lax.all_to_all(tiles, "dy", split_axis=0, concat_axis=0, tiled=True)
    return arrived.astype(F32).sum(axis=0)


def shards(value_grad, stream, weights, gain, top_grad, counts):
    section_index = lax.axis_index("section")
    model_index = lax.axis_index(MP)
    place = lax.axis_index("dz")
    scal = jnp.stack([place, 1 - 2 * (place % 2), model_index, counts[0]]).astype(jnp.int32)
    held, stats, own, *blocks = front(scal, stream[0], value_grad[0], gain)
    tiles = parts(value_grad[0], weights[0], held, gain, stats)
    weight_grad = sum_over_y(sum_over_z(own, blocks, tiles)).astype(BF16)[None]
    arrived = lax.all_to_all(tiles, MP, split_axis=0, concat_axis=0, tiled=True)
    norm_back, above_grad = backward(scal, arrived, stats, gain, top_grad, stream[0])
    below_grad = lax.ppermute(above_grad, "section", [(1, 0)])
    lower_grad = (below_grad.astype(F32) + norm_back).astype(BF16)
    result = jnp.where(section_index == 0, lower_grad, above_grad)
    return (weight_grad, result[None])


def solution(mesh):
    split = Mesh(
        mesh.devices.reshape(mesh.shape["section"], 2, 4, 12, 4),
        ("section", "my", "mx", "dz", "dy"),
    )
    placed = (
        P("section", DP, MP),
        P("section", DP, None),
        P("section", MP, None),
        P("section", None),
        P(DP, None),
        P(DP),
    )

    return jax.shard_map(
        shards,
        mesh=split,
        in_specs=placed,
        out_specs=(P("section", MP + DP, None), P("section", DP, MP)),
        check_vma=False,
    )
```

```python
import jax
import jax.numpy as jnp
from jax import lax
from jax.experimental import pallas as pl
from jax.experimental.pallas import tpu as pltpu
from jax.sharding import Mesh
from jax.sharding import PartitionSpec as P


TOK_MB = 256
DP = ("dz", "dy")
MP = ("my", "mx")
F32 = jnp.float32
BF16 = jnp.bfloat16
TOK = 512
BLOCK = 128
CHUNK = 16
UNROLL = 8
WIDTH = 3072
SHARE = 384
RING = 12
ROWS = SHARE // RING
PARTS = 8
EXTRA = 8
COLS = 512


def in_hbm(*arrays):
    return [pltpu.with_memory_space_constraint(a, pltpu.HBM) for a in arrays]


def front_kernel(counts, stream, value_grad_from, gain_from, held, stats, own, *rest):
    blocks, (normed, grad, value_grad, gain, sems) = rest[:-5], rest[-5:]
    place = lax.axis_index("dz")
    ahead = 1 - 2 * lax.rem(place, 2)
    per = TOK // BLOCK
    gain_here = pltpu.make_async_copy(gain_from, gain, sems.at[per])
    gain_here.start()
    arrivals = []
    for b in range(TOK // BLOCK):
        rows = pl.ds(b * BLOCK, BLOCK)
        arrivals.append(pltpu.make_async_copy(stream.at[rows, :], held.at[rows, :], sems.at[b]))
        arrivals[-1].start()
    value_grad_here = pltpu.make_async_copy(value_grad_from, value_grad, sems.at[per + 1])
    value_grad_here.start()
    gain_here.wait()
    lanes = [slice(t * 128, (t + 1) * 128) for t in range(WIDTH // 128)]

    def chunk(i, carry):
        rows = pl.ds(pl.multiple_of(i * CHUNK, CHUNK), CHUNK)
        total = [jnp.zeros((CHUNK, 128), F32)] * 2
        for t, lane in enumerate(lanes):
            total[t % 2] += held[rows, lane].astype(F32)
        mean = jnp.sum(total[0] + total[1], axis=1, keepdims=True) * (1.0 / WIDTH)
        total = [jnp.zeros((CHUNK, 128), F32)] * 2
        for t, lane in enumerate(lanes):
            centred = held[rows, lane].astype(F32) - mean
            total[t % 2] += centred * centred
        variance = jnp.sum(total[0] + total[1], axis=1, keepdims=True) * (1.0 / WIDTH)
        inv = lax.rsqrt(variance + 1e-06)
        for lane in lanes:
            normed[rows, lane] = ((held[rows, lane].astype(F32) - mean) * inv * gain[:, lane]).astype(BF16)
        stats[0, rows, :] = jnp.broadcast_to(inv, (CHUNK, 128))
        stats[1, rows, :] = jnp.broadcast_to(mean, (CHUNK, 128))
        return carry

    per = BLOCK // CHUNK
    for b in range(TOK // BLOCK):
        arrivals[b].wait()
        lax.fori_loop(b * per, (b + 1) * per, chunk, 0, unroll=UNROLL)
    value_grad_here.wait()
    token = lax.broadcasted_iota(jnp.int32, (TOK, SHARE), 0)
    live = token < counts[0] * TOK_MB
    left = jnp.where(live, value_grad[...].astype(F32), 0.0).astype(BF16).T
    for n in range(WIDTH // COLS):
        cols = slice(n * COLS, (n + 1) * COLS)
        grad[...] = jnp.dot(left, normed[:, cols], preferred_element_type=F32)
        for r in range(RING):
            at = lax.rem(place + r * ahead + RING, RING) * ROWS
            piece = grad[pl.ds(pl.multiple_of(at, ROWS), ROWS), :]
            if r == 0:
                own[:, cols] = piece
            else:
                blocks[r - 1][:, cols] = piece.astype(BF16)


def front(stream, value_grad, gain, counts):
    vmem = pl.BlockSpec(memory_space=pltpu.VMEM)
    out = [((TOK, WIDTH), BF16), ((2, TOK, 128), F32), ((ROWS, WIDTH), F32)]
    out += [((ROWS, WIDTH), BF16)] * (RING - 1)
    return pl.pallas_call(
        front_kernel,
        in_specs=[
            pl.BlockSpec(memory_space=pltpu.SMEM),
            *[pl.BlockSpec(memory_space=pl.ANY)] * 3,
        ],
        out_specs=[vmem] * len(out),
        scratch_shapes=[
            pltpu.VMEM((TOK, WIDTH), BF16),
            pltpu.VMEM((SHARE, COLS), F32),
            pltpu.VMEM((TOK, SHARE), BF16),
            pltpu.VMEM((1, WIDTH), F32),
            pltpu.SemaphoreType.DMA((TOK // BLOCK + 2,)),
        ],
        out_shape=[jax.ShapeDtypeStruct(*o) for o in out],
        compiler_params=pltpu.CompilerParams(vmem_limit_bytes=24 * 1024 * 1024),
        cost_estimate=pl.CostEstimate(flops=2 * TOK * SHARE * WIDTH * 4, transcendentals=0, bytes_accessed=8_000_000),
    )(counts, *in_hbm(stream, value_grad, gain))


def parts_kernel(value_grad, weights, held, gain, stats, out, packed, extra, sums, sems):
    copies = []
    for m in range(PARTS):
        cols = slice(m * SHARE, (m + 1) * SHARE)
        part = jnp.dot(value_grad[...], weights[:, cols], preferred_element_type=F32).astype(BF16)
        packed[m] = part
        copies.append(pltpu.make_async_copy(packed.at[m], out.at[m, pl.ds(0, TOK), :], sems.at[m]))
        copies[-1].start()
        scaled = part.astype(F32) * gain[:, cols]
        tiles = [scaled[:, t * 128 : (t + 1) * 128] for t in range(SHARE // 128)]
        first = tiles[0] + tiles[1] + tiles[2]
        second = None
        for t, tile in enumerate(tiles):
            low = m * SHARE + t * 128
            term = tile * (held[:, low : low + 128].astype(F32) - stats[1])
            second = term if second is None else second + term
        if m == 0:
            sums[0] = first
            sums[1] = second
        else:
            sums[0] += first
            sums[1] += second
    lines = []
    for total in (sums[0], sums[1] * stats[0]):
        line = jnp.sum(total.T, axis=0, keepdims=True)
        high = line.astype(BF16).astype(F32)
        lines += [high, line - high]
    stacked = jnp.concatenate(lines, axis=0)
    tail = jnp.concatenate([stacked[:, SHARE:], jnp.zeros((4, SHARE - 128), F32)], axis=1)
    extra[...] = jnp.concatenate([stacked[:, :SHARE], tail], axis=0).astype(BF16)
    for m in range(PARTS):
        copies.append(pltpu.make_async_copy(extra, out.at[m, pl.ds(TOK, EXTRA), :], sems.at[PARTS + m]))
        copies[-1].start()
    for copy in copies:
        copy.wait()


def parts(value_grad, weights, held, gain, stats):
    vmem = pl.BlockSpec(memory_space=pltpu.VMEM)
    return pl.pallas_call(
        parts_kernel,
        in_specs=[vmem] * 5,
        out_specs=pl.BlockSpec(memory_space=pl.ANY),
        out_shape=pltpu.HBM((PARTS, TOK + EXTRA, SHARE), BF16),
        scratch_shapes=[
            pltpu.VMEM((PARTS, TOK, SHARE), BF16),
            pltpu.VMEM((EXTRA, SHARE), BF16),
            pltpu.VMEM((2, TOK, 128), F32),
            pltpu.SemaphoreType.DMA((2 * PARTS,)),
        ],
        compiler_params=pltpu.CompilerParams(vmem_limit_bytes=16 * 1024 * 1024),
        cost_estimate=pl.CostEstimate(flops=2 * TOK * SHARE * WIDTH * 3, transcendentals=0, bytes_accessed=9_000_000),
    )(value_grad, weights, held, gain, stats)


def back_kernel(sent, stats, gain, top, stream, back, above, arrived, top_here, stream_here, columns, sems):
    model_index = lax.axis_index("my") * 4 + lax.axis_index("mx")
    share = pl.ds(pl.multiple_of(model_index * SHARE, 128), SHARE)
    fetches = [
        pltpu.make_async_copy(stream.at[:, share], stream_here, sems.at[0]),
        pltpu.make_async_copy(top.at[:, share], top_here, sems.at[1]),
    ]
    rows_of = [pl.ds(TOK, EXTRA)] + [pl.ds(b * BLOCK, BLOCK) for b in range(TOK // BLOCK)]
    for i, rows in enumerate(rows_of):
        fetches.append(pltpu.make_async_copy(sent.at[:, rows, :], arrived.at[:, rows, :], sems.at[2 + i]))
    for i in (2, 0, 1, 3, 4, 5, 6):
        fetches[i].start()
    fetches[2].wait()
    sums = jnp.sum(arrived[:, TOK:, :].astype(F32), axis=0)
    lines = jnp.concatenate([sums[:4], sums[4:, :128]], axis=1)
    for j, line in enumerate((lines[0:1] + lines[1:2], lines[2:3] + lines[3:4])):
        for b in range(TOK // BLOCK):
            square = jnp.broadcast_to(line[:, b * BLOCK : (b + 1) * BLOCK], (BLOCK, BLOCK))
            columns[j, b * BLOCK : (b + 1) * BLOCK, :] = square.T * (1.0 / WIDTH)
    gains = gain[:, share]
    fetches[0].wait()
    fetches[1].wait()

    def chunk(i, carry):
        rows = pl.ds(pl.multiple_of(i * CHUNK, CHUNK), CHUNK)
        total = arrived[0, rows, :].astype(F32)
        for j in range(1, PARTS):
            total = total + arrived[j, rows, :].astype(F32)
        spread = lambda a: jnp.concatenate([a] * (SHARE // 128), axis=1)
        scale = spread(stats[0, rows, :])
        white = (stream_here[rows, :].astype(F32) - spread(stats[1, rows, :])) * scale
        branch = scale * (total * gains - spread(columns[0, rows, :]) - white * spread(columns[1, rows, :]))
        back[rows, :] = branch
        above[rows, :] = (top_here[rows, :].astype(F32) + branch).astype(BF16)
        return carry

    per = BLOCK // CHUNK
    for b in range(TOK // BLOCK):
        fetches[3 + b].wait()
        lax.fori_loop(b * per, (b + 1) * per, chunk, 0, unroll=4)


def backward(arrived, stats, gain, top, stream):
    vmem = pl.BlockSpec(memory_space=pltpu.VMEM)
    hbm = pl.BlockSpec(memory_space=pl.ANY)
    return pl.pallas_call(
        back_kernel,
        in_specs=[hbm, vmem, vmem, hbm, hbm],
        out_specs=[vmem, vmem],
        scratch_shapes=[
            pltpu.VMEM((PARTS, TOK + EXTRA, SHARE), BF16),
            pltpu.VMEM((TOK, SHARE), BF16),
            pltpu.VMEM((TOK, SHARE), BF16),
            pltpu.VMEM((2, TOK, BLOCK), F32),
            pltpu.SemaphoreType.DMA((2 + 1 + TOK // BLOCK,)),
        ],
        out_shape=[jax.ShapeDtypeStruct((TOK, SHARE), F32), jax.ShapeDtypeStruct((TOK, SHARE), BF16)],
        compiler_params=pltpu.CompilerParams(vmem_limit_bytes=12 * 1024 * 1024),
        cost_estimate=pl.CostEstimate(flops=500_000_000, transcendentals=0, bytes_accessed=6_000_000),
    )(*in_hbm(arrived), stats, gain, *in_hbm(top, stream))


def swapped(value, link):
    peers = lax.axis_size("dz")
    pairs = []
    for i in range(link, peers, 2):
        pairs += [(i, (i + 1) % peers), ((i + 1) % peers, i)]
    return lax.ppermute(value, "dz", pairs)


def tied(value, *others):
    return lax.optimization_barrier((value, *others))[0]


def joined_kernel(own, got, out):
    out[...] = (own[...].astype(F32) + got[...].astype(F32)).astype(BF16)


def joined(own, got):
    vmem = pl.BlockSpec(memory_space=pltpu.VMEM)
    return pl.pallas_call(
        joined_kernel,
        in_specs=[vmem, vmem],
        out_specs=vmem,
        out_shape=jax.ShapeDtypeStruct(own.shape, BF16),
        compiler_params=pltpu.CompilerParams(vmem_limit_bytes=4 * 1024 * 1024),
    )(own, got)


def sum_over_z(own, blocks, after):
    def block(link, distance):
        return blocks[(distance if link == 0 else RING - distance) - 1]

    far = RING // 2
    long = swapped(block(0, far), 0)
    short = None
    link = 0
    for k in range(far - 1, 0, -1):
        link = 1 - link
        if short is None:
            mine_short = tied(block(1 - link, k), after)
        else:
            mine_short = joined(block(1 - link, k), short)
            long = tied(long, short)
        short = swapped(mine_short, 1 - link)
        mine = joined(block(link, k), long)
        long = swapped(mine, link)
    return own + long.astype(F32) + short.astype(F32)


def sum_over_y(rows_sum):
    peers = lax.axis_size("dy")
    tiles = rows_sum.astype(BF16).reshape(peers, rows_sum.shape[0] // peers, rows_sum.shape[1])
    arrived = lax.all_to_all(tiles, "dy", split_axis=0, concat_axis=0, tiled=True)
    return arrived.astype(F32).sum(axis=0)


def shards(value_grad, stream, weights, gain, top_grad, counts):
    section_index = lax.axis_index("section")
    held, stats, own, *blocks = front(stream[0], value_grad[0], gain, counts)
    tiles = parts(value_grad[0], weights[0], held, gain, stats)
    weight_grad = sum_over_y(sum_over_z(own, blocks, tiles)).astype(BF16)[None]
    arrived = lax.all_to_all(tiles, MP, split_axis=0, concat_axis=0, tiled=True)
    norm_back, above_grad = backward(arrived, stats, gain, top_grad, stream[0])
    below_grad = lax.ppermute(above_grad, "section", [(1, 0)])
    lower_grad = (below_grad.astype(F32) + norm_back).astype(BF16)
    result = jnp.where(section_index == 0, lower_grad, above_grad)
    return (weight_grad, result[None])


def solution(mesh):
    split = Mesh(
        mesh.devices.reshape(mesh.shape["section"], 2, 4, 12, 4),
        ("section", "my", "mx", "dz", "dy"),
    )
    placed = (
        P("section", DP, MP),
        P("section", DP, None),
        P("section", MP, None),
        P("section", None),
        P(DP, None),
        P(DP),
    )

    return jax.shard_map(
        shards,
        mesh=split,
        in_specs=placed,
        out_specs=(P("section", MP + DP, None), P("section", DP, MP)),
        check_vma=False,
    )
```

```python
import jax
import jax.numpy as jnp
from jax import lax
from jax.experimental import pallas as pl
from jax.experimental.pallas import tpu as pltpu
from jax.sharding import Mesh
from jax.sharding import PartitionSpec as P


TOK_MB = 256
DP = ("dz", "dy")
MP = ("my", "mx")
F32 = jnp.float32
BF16 = jnp.bfloat16
TOK = 512
BLOCK = 128
CHUNK = 16
UNROLL = 8
WIDTH = 3072
SHARE = 384
RING = 12
ROWS = SHARE // RING
PARTS = 8
EXTRA = 8
COLS = 512


def in_hbm(*arrays):
    return [pltpu.with_memory_space_constraint(a, pltpu.HBM) for a in arrays]


def front_kernel(counts, stream, value_grad_from, gain_from, held, stats, own, *rest):
    blocks, (normed, grad, value_grad, gain, sems) = rest[:-5], rest[-5:]
    place = lax.axis_index("dz")
    ahead = 1 - 2 * lax.rem(place, 2)
    per = TOK // BLOCK
    gain_here = pltpu.make_async_copy(gain_from, gain, sems.at[per])
    gain_here.start()
    arrivals = []
    for b in range(TOK // BLOCK):
        rows = pl.ds(b * BLOCK, BLOCK)
        arrivals.append(pltpu.make_async_copy(stream.at[rows, :], held.at[rows, :], sems.at[b]))
        arrivals[-1].start()
    value_grad_here = pltpu.make_async_copy(value_grad_from, value_grad, sems.at[per + 1])
    value_grad_here.start()
    gain_here.wait()
    lanes = [slice(t * 128, (t + 1) * 128) for t in range(WIDTH // 128)]

    def chunk(i, carry):
        rows = pl.ds(pl.multiple_of(i * CHUNK, CHUNK), CHUNK)
        total = [jnp.zeros((CHUNK, 128), F32)] * 2
        for t, lane in enumerate(lanes):
            total[t % 2] += held[rows, lane].astype(F32)
        mean = jnp.sum(total[0] + total[1], axis=1, keepdims=True) * (1.0 / WIDTH)
        total = [jnp.zeros((CHUNK, 128), F32)] * 2
        for t, lane in enumerate(lanes):
            centred = held[rows, lane].astype(F32) - mean
            total[t % 2] += centred * centred
        variance = jnp.sum(total[0] + total[1], axis=1, keepdims=True) * (1.0 / WIDTH)
        inv = lax.rsqrt(variance + 1e-06)
        for lane in lanes:
            normed[rows, lane] = ((held[rows, lane].astype(F32) - mean) * inv * gain[:, lane]).astype(BF16)
        stats[0, rows, :] = jnp.broadcast_to(inv, (CHUNK, 128))
        stats[1, rows, :] = jnp.broadcast_to(mean, (CHUNK, 128))
        return carry

    per = BLOCK // CHUNK
    for b in range(TOK // BLOCK):
        arrivals[b].wait()
        lax.fori_loop(b * per, (b + 1) * per, chunk, 0, unroll=UNROLL)
    value_grad_here.wait()
    token = lax.broadcasted_iota(jnp.int32, (TOK, SHARE), 0)
    live = token < counts[0] * TOK_MB
    left = jnp.where(live, value_grad[...].astype(F32), 0.0).astype(BF16).T
    for n in range(WIDTH // COLS):
        cols = slice(n * COLS, (n + 1) * COLS)
        grad[...] = jnp.dot(left, normed[:, cols], preferred_element_type=F32)
        for r in range(RING):
            at = lax.rem(place + r * ahead + RING, RING) * ROWS
            piece = grad[pl.ds(pl.multiple_of(at, ROWS), ROWS), :]
            if r == 0:
                own[:, cols] = piece
            else:
                blocks[r - 1][:, cols] = piece.astype(BF16)


def front(stream, value_grad, gain, counts):
    vmem = pl.BlockSpec(memory_space=pltpu.VMEM)
    out = [((TOK, WIDTH), BF16), ((2, TOK, 128), F32), ((ROWS, WIDTH), F32)]
    out += [((ROWS, WIDTH), BF16)] * (RING - 1)
    return pl.pallas_call(
        front_kernel,
        in_specs=[
            pl.BlockSpec(memory_space=pltpu.SMEM),
            *[pl.BlockSpec(memory_space=pl.ANY)] * 3,
        ],
        out_specs=[vmem] * len(out),
        scratch_shapes=[
            pltpu.VMEM((TOK, WIDTH), BF16),
            pltpu.VMEM((SHARE, COLS), F32),
            pltpu.VMEM((TOK, SHARE), BF16),
            pltpu.VMEM((1, WIDTH), F32),
            pltpu.SemaphoreType.DMA((TOK // BLOCK + 2,)),
        ],
        out_shape=[jax.ShapeDtypeStruct(*o) for o in out],
        compiler_params=pltpu.CompilerParams(vmem_limit_bytes=24 * 1024 * 1024),
        cost_estimate=pl.CostEstimate(flops=2 * TOK * SHARE * WIDTH * 4, transcendentals=0, bytes_accessed=8_000_000),
    )(counts, *in_hbm(stream, value_grad, gain))


def parts_kernel(value_grad, weights, held, gain, stats, out, packed, extra, sums, sems):
    copies = []
    for m in range(PARTS):
        cols = slice(m * SHARE, (m + 1) * SHARE)
        part = jnp.dot(value_grad[...], weights[:, cols], preferred_element_type=F32).astype(BF16)
        packed[m] = part
        copies.append(pltpu.make_async_copy(packed.at[m], out.at[m, pl.ds(0, TOK), :], sems.at[m]))
        copies[-1].start()
        scaled = part.astype(F32) * gain[:, cols]
        tiles = [scaled[:, t * 128 : (t + 1) * 128] for t in range(SHARE // 128)]
        first = tiles[0] + tiles[1] + tiles[2]
        second = None
        for t, tile in enumerate(tiles):
            low = m * SHARE + t * 128
            term = tile * (held[:, low : low + 128].astype(F32) - stats[1])
            second = term if second is None else second + term
        if m == 0:
            sums[0] = first
            sums[1] = second
        else:
            sums[0] += first
            sums[1] += second
    lines = []
    for total in (sums[0], sums[1] * stats[0]):
        line = jnp.sum(total.T, axis=0, keepdims=True)
        high = line.astype(BF16).astype(F32)
        lines += [high, line - high]
    stacked = jnp.concatenate(lines, axis=0)
    tail = jnp.concatenate([stacked[:, SHARE:], jnp.zeros((4, SHARE - 128), F32)], axis=1)
    extra[...] = jnp.concatenate([stacked[:, :SHARE], tail], axis=0).astype(BF16)
    for m in range(PARTS):
        copies.append(pltpu.make_async_copy(extra, out.at[m, pl.ds(TOK, EXTRA), :], sems.at[PARTS + m]))
        copies[-1].start()
    for copy in copies:
        copy.wait()


def parts(value_grad, weights, held, gain, stats):
    vmem = pl.BlockSpec(memory_space=pltpu.VMEM)
    return pl.pallas_call(
        parts_kernel,
        in_specs=[vmem] * 5,
        out_specs=pl.BlockSpec(memory_space=pl.ANY),
        out_shape=pltpu.HBM((PARTS, TOK + EXTRA, SHARE), BF16),
        scratch_shapes=[
            pltpu.VMEM((PARTS, TOK, SHARE), BF16),
            pltpu.VMEM((EXTRA, SHARE), BF16),
            pltpu.VMEM((2, TOK, 128), F32),
            pltpu.SemaphoreType.DMA((2 * PARTS,)),
        ],
        compiler_params=pltpu.CompilerParams(vmem_limit_bytes=16 * 1024 * 1024),
        cost_estimate=pl.CostEstimate(flops=2 * TOK * SHARE * WIDTH * 3, transcendentals=0, bytes_accessed=9_000_000),
    )(value_grad, weights, held, gain, stats)


def back_kernel(sent, stats, gain, top, stream, back, above, arrived, top_here, stream_here, columns, sems):
    model_index = lax.axis_index("my") * 4 + lax.axis_index("mx")
    share = pl.ds(pl.multiple_of(model_index * SHARE, 128), SHARE)
    fetches = [
        pltpu.make_async_copy(stream.at[:, share], stream_here, sems.at[0]),
        pltpu.make_async_copy(top.at[:, share], top_here, sems.at[1]),
    ]
    rows_of = [pl.ds(TOK, EXTRA)] + [pl.ds(b * BLOCK, BLOCK) for b in range(TOK // BLOCK)]
    for i, rows in enumerate(rows_of):
        fetches.append(pltpu.make_async_copy(sent.at[:, rows, :], arrived.at[:, rows, :], sems.at[2 + i]))
    for i in (2, 0, 1, 3, 4, 5, 6):
        fetches[i].start()
    fetches[2].wait()
    sums = jnp.sum(arrived[:, TOK:, :].astype(F32), axis=0)
    lines = jnp.concatenate([sums[:4], sums[4:, :128]], axis=1)
    for j, line in enumerate((lines[0:1] + lines[1:2], lines[2:3] + lines[3:4])):
        for b in range(TOK // BLOCK):
            square = jnp.broadcast_to(line[:, b * BLOCK : (b + 1) * BLOCK], (BLOCK, BLOCK))
            columns[j, b * BLOCK : (b + 1) * BLOCK, :] = square.T * (1.0 / WIDTH)
    gains = gain[:, share]
    fetches[0].wait()
    fetches[1].wait()

    def chunk(i, carry):
        rows = pl.ds(pl.multiple_of(i * CHUNK, CHUNK), CHUNK)
        total = arrived[0, rows, :].astype(F32)
        for j in range(1, PARTS):
            total = total + arrived[j, rows, :].astype(F32)
        spread = lambda a: jnp.concatenate([a] * (SHARE // 128), axis=1)
        scale = spread(stats[0, rows, :])
        white = (stream_here[rows, :].astype(F32) - spread(stats[1, rows, :])) * scale
        branch = scale * (total * gains - spread(columns[0, rows, :]) - white * spread(columns[1, rows, :]))
        back[rows, :] = branch
        above[rows, :] = (top_here[rows, :].astype(F32) + branch).astype(BF16)
        return carry

    per = BLOCK // CHUNK
    for b in range(TOK // BLOCK):
        fetches[3 + b].wait()
        lax.fori_loop(b * per, (b + 1) * per, chunk, 0, unroll=4)


def backward(arrived, stats, gain, top, stream):
    vmem = pl.BlockSpec(memory_space=pltpu.VMEM)
    hbm = pl.BlockSpec(memory_space=pl.ANY)
    return pl.pallas_call(
        back_kernel,
        in_specs=[hbm, vmem, vmem, hbm, hbm],
        out_specs=[vmem, vmem],
        scratch_shapes=[
            pltpu.VMEM((PARTS, TOK + EXTRA, SHARE), BF16),
            pltpu.VMEM((TOK, SHARE), BF16),
            pltpu.VMEM((TOK, SHARE), BF16),
            pltpu.VMEM((2, TOK, BLOCK), F32),
            pltpu.SemaphoreType.DMA((2 + 1 + TOK // BLOCK,)),
        ],
        out_shape=[jax.ShapeDtypeStruct((TOK, SHARE), F32), jax.ShapeDtypeStruct((TOK, SHARE), BF16)],
        compiler_params=pltpu.CompilerParams(vmem_limit_bytes=12 * 1024 * 1024),
        cost_estimate=pl.CostEstimate(flops=500_000_000, transcendentals=0, bytes_accessed=6_000_000),
    )(*in_hbm(arrived), stats, gain, *in_hbm(top, stream))


def swapped(value, link):
    peers = lax.axis_size("dz")
    pairs = []
    for i in range(link, peers, 2):
        pairs += [(i, (i + 1) % peers), ((i + 1) % peers, i)]
    return lax.ppermute(value, "dz", pairs)


def tied(value, *others):
    return lax.optimization_barrier((value, *others))[0]


def joined_kernel(own, got, out):
    out[...] = (own[...].astype(F32) + got[...].astype(F32)).astype(BF16)


def joined(own, got):
    vmem = pl.BlockSpec(memory_space=pltpu.VMEM)
    return pl.pallas_call(
        joined_kernel,
        in_specs=[vmem, vmem],
        out_specs=vmem,
        out_shape=jax.ShapeDtypeStruct(own.shape, BF16),
        compiler_params=pltpu.CompilerParams(vmem_limit_bytes=4 * 1024 * 1024),
    )(own, got)


def sum_over_z(own, blocks, after):
    def block(link, distance):
        return blocks[(distance if link == 0 else RING - distance) - 1]

    far = RING // 2
    long = swapped(block(0, far), 0)
    short = None
    link = 0
    for k in range(far - 1, 0, -1):
        link = 1 - link
        if short is None:
            mine_short = tied(block(1 - link, k), after)
        else:
            mine_short = joined(block(1 - link, k), short)
            long = tied(long, short)
        short = swapped(mine_short, 1 - link)
        mine = joined(block(link, k), long)
        long = swapped(mine, link)
    vmem = pl.BlockSpec(memory_space=pltpu.VMEM)
    peers = lax.axis_size("dy")
    return pl.pallas_call(
        total_kernel,
        in_specs=[vmem] * 3,
        out_specs=vmem,
        out_shape=jax.ShapeDtypeStruct((peers, ROWS // peers, WIDTH), BF16),
        compiler_params=pltpu.CompilerParams(vmem_limit_bytes=4 * 1024 * 1024),
    )(own, long, short)


def total_kernel(own, long, short, out):
    for i in range(out.shape[0]):
        rows = slice(i * out.shape[1], (i + 1) * out.shape[1])
        out[i] = (own[rows, :] + long[rows, :].astype(F32) + short[rows, :].astype(F32)).astype(BF16)


def sum_over_y(tiles):
    arrived = lax.all_to_all(tiles, "dy", split_axis=0, concat_axis=0, tiled=True)
    return arrived.astype(F32).sum(axis=0)


def shards(value_grad, stream, weights, gain, top_grad, counts):
    section_index = lax.axis_index("section")
    held, stats, own, *blocks = front(stream[0], value_grad[0], gain, counts)
    tiles = parts(value_grad[0], weights[0], held, gain, stats)
    weight_grad = sum_over_y(sum_over_z(own, blocks, tiles)).astype(BF16)[None]
    arrived = lax.all_to_all(tiles, MP, split_axis=0, concat_axis=0, tiled=True)
    norm_back, above_grad = backward(arrived, stats, gain, top_grad, stream[0])
    below_grad = lax.ppermute(above_grad, "section", [(1, 0)])
    lower_grad = (below_grad.astype(F32) + norm_back).astype(BF16)
    result = jnp.where(section_index == 0, lower_grad, above_grad)[None]
    return (weight_grad, result)


def solution(mesh):
    split = Mesh(
        mesh.devices.reshape(mesh.shape["section"], 2, 4, 12, 4),
        ("section", "my", "mx", "dz", "dy"),
    )
    placed = (
        P("section", DP, MP),
        P("section", DP, None),
        P("section", MP, None),
        P("section", None),
        P(DP, None),
        P(DP),
    )

    return jax.shard_map(
        shards,
        mesh=split,
        in_specs=placed,
        out_specs=(P("section", MP + DP, None), P("section", DP, MP)),
        check_vma=False,
    )
```
